32 devices in a mesh: dp: 8 (over z, core), tp: 4 (over y, x).
Axes of the slice: x: 2, y: 2, z: 4, core: 2. Of those that a mesh axis runs over, the one named last changes fastest.
Arguments:
- tokens: bfloat16 [4096, 4096], P('dp'), may hold values from -6 to 6
- gain: float32 [4096], replicated, may hold values from 0.1 to 1.9
- router: float32 [4096, 8], replicated, may hold values from -0.09375 to 0.09375
- routes: int32 [4096, 2], P('dp'), may hold values from 0 to 7, all different within a row
- w_gate: bfloat16 [2, 4096, 1024], P(None, 'dp', 'tp'), may hold values from -0.125 to 0.125
- w_up: bfloat16 [2, 4096, 1024], P(None, 'dp', 'tp'), may hold values from -0.125 to 0.125
- w_down: bfloat16 [2, 1024, 4096], P(None, 'dp', 'tp'), may hold values from -0.25 to 0.25
Outputs:
- mixed: bfloat16 [4096, 4096], P('dp', 'tp')
The draws below stay inside these ranges and needn't reach their ends.
Inputs may be any that keep to these rules, and one draw needn't show every extreme that they name: `routes`: each row names two different experts.
All inputs are finite; a program needn't handle non-finite values.
Results may differ from the reference program's by a relative error of at most 0.0065.
Values may be sent and summed in bfloat16 or wider, within the bound.
A program may use at most 64 MiB of HBM per device.

```python
import jax
import jax.numpy as jnp
from jax import lax

D = 4096
FF = 1024
EXP = 2
ROUTED = 8
TOK_GRP = 512
TOKENS = 4096


def raised(array, own_key, source, target, blocks, factor):
    def block_of(axis_at):
        return (jnp.arange(array.shape[axis_at]) // (array.shape[axis_at] // blocks)).reshape((-1,) + (1,) * (array.ndim - 1 - axis_at))

    near = jax.random.permutation(own_key, blocks)[block_of(target)]
    second = (block_of(target) + blocks // 2) % blocks
    return jnp.where((block_of(source) == near) | (block_of(source) == second), factor * array, array)


def steps_of(rng, shape, shards, smallest, largest):
    level = 1.0
    for dim, blocks in shards:
        steps = jax.random.uniform(jax.random.fold_in(jax.random.fold_in(rng, 6), dim), (blocks,), jnp.float32, smallest / len(shards), largest / len(shards))
        level = level * jnp.repeat(jnp.exp(steps), shape[dim] // blocks).reshape((-1,) + (1,) * (len(shape) - 1 - dim))
    return level


def different_ones(rng, rows, amount, top, lift):
    sequence = jax.random.permutation(jax.random.fold_in(rng, 1), amount)
    favour = sequence
    for power in range(3):
        favour = favour * favour // amount
    favour = favour * lift // amount
    lots = jax.random.randint(jax.random.fold_in(rng, 2), (rows, amount), 0, 4096) + favour
    fixed_rows = jax.random.permutation(jax.random.fold_in(rng, 3), rows)[jnp.arange(amount) % rows]
    lots = jnp.where(jnp.arange(rows)[:, None] == fixed_rows[None, :], 1 << 14, lots)
    score = lots * amount + jnp.arange(amount)
    return lax.top_k(score.astype(jnp.int32), top)[1].astype(jnp.int32)


def noise(own_key, shape, deviation, reach, split=(), kind=jnp.bfloat16):
    level = steps_of(own_key, shape, split, -0.22, 0.18) if split else 1.0
    values = jax.random.normal(own_key, shape, jnp.float32) * deviation * level
    return jnp.minimum(jnp.maximum(values, -reach), reach).astype(kind)


def heavy_noise(rng, shape, width, most, cuts, heavy, kind=jnp.bfloat16):
    drawn = width * jax.random.normal(rng, shape, jnp.float32)
    if cuts:
        drawn = drawn * steps_of(rng, shape, cuts, -0.22, 0.18)
    return jnp.clip(raised(drawn, jax.random.fold_in(rng, 3), *heavy), -most, most).astype(kind)


def setup_inputs(seed: int = 0) -> dict:
    keys = jax.random.split(jax.random.key(seed), 8)
    return {
        "tokens": noise(keys[0], (TOKENS, D), 1.0, 6.0, ((0, 8),)),
        "gain": jnp.clip(1.0 + 0.18 * jax.random.normal(keys[1], (D,), jnp.float32), 0.1, 1.9),
        "router": noise(keys[2], (D, ROUTED), D ** -0.5, 0.09375, (), jnp.float32),
        "routes": different_ones(keys[3], TOKENS, ROUTED, 2, 2048),
        "w_gate": heavy_noise(keys[4], (EXP, D, FF), D ** -0.5, 0.125, ((1, 8), (2, 4)), (1, 2, 8, 2.0)),
        "w_up": heavy_noise(keys[5], (EXP, D, FF), D ** -0.5, 0.125, ((1, 8), (2, 4)), (1, 2, 8, 2.0)),
        "w_down": heavy_noise(keys[6], (EXP, FF, D), FF ** -0.5, 0.25, ((1, 8), (2, 4)), (1, 2, 8, 2.0)),
    }


EPS = 1e-06
ROUTE_SCALE = 2.5

def one_group(tokens, gain, router, routes, w_gate, w_up, w_down):
    values = tokens.astype(jnp.float32)
    square = lax.optimization_barrier(jnp.mean(values * values, axis=-1, keepdims=True))
    normed = (values * lax.rsqrt(square + EPS) * gain).astype(jnp.bfloat16)
    scores = jax.nn.sigmoid(jnp.dot(normed.astype(jnp.float32), router, precision=lax.Precision.HIGHEST))
    labels = jnp.arange(router.shape[1], dtype=jnp.int32)
    picked_mask = (routes[:, :, None] == labels[None, None, :]).astype(jnp.float32)
    picked = lax.optimization_barrier(jnp.sum(picked_mask * scores[:, None, :], axis=-1))
    chosen = lax.optimization_barrier(jnp.sum(picked_mask, axis=1))
    combine = chosen * scores * ROUTE_SCALE / lax.optimization_barrier(jnp.sum(picked, axis=-1, keepdims=True))
    total = jnp.zeros((tokens.shape[0], w_down.shape[2]), jnp.float32)
    for expert in range(w_gate.shape[0]):
        gate_value = jnp.dot(normed, w_gate[expert], preferred_element_type=jnp.float32)
        up_value = jnp.dot(normed, w_up[expert], preferred_element_type=jnp.float32)
        hidden = (jax.nn.silu(gate_value) * up_value * combine[:, expert:expert + 1]).astype(jnp.bfloat16)
        total = total + jnp.dot(hidden, w_down[expert], preferred_element_type=jnp.float32)
    return total.astype(jnp.bfloat16)

def reference(tokens, gain, router, routes, w_gate, w_up, w_down):
    groups = tokens.shape[0] // TOK_GRP
    grouped = tokens.reshape(groups, TOK_GRP, tokens.shape[1])
    grouped_routes = routes.reshape(groups, TOK_GRP, 2)

    def apply(pair):
        return one_group(pair[0], gain, router, pair[1], w_gate, w_up, w_down)
    mixed = lax.map(apply, (grouped, grouped_routes))
    return mixed.reshape(tokens.shape[0], w_down.shape[2])
```

```python
import functools

import jax
import jax.numpy as jnp
from jax import lax
from jax.experimental import pallas as pl
from jax.experimental.pallas import tpu as pltpu
from jax.sharding import PartitionSpec as P

EPS = 1e-06
ROUTE_SCALE = 2.5
MESH = pl.DeviceIdType.MESH
CORES = 2


def gathered(tokens, gain, router, routes, w_gate, w_up, w_down):
    values = tokens.astype(jnp.float32)
    square = jnp.mean(values * values, axis=-1, keepdims=True)
    normed = (values * lax.rsqrt(square + EPS) * gain).astype(jnp.bfloat16)
    scores = jax.nn.sigmoid(
        jnp.dot(normed.astype(jnp.float32), router, precision=lax.Precision.HIGHEST)
    )
    labels = jnp.arange(router.shape[1], dtype=jnp.int32)
    picked_mask = (routes[:, :, None] == labels[None, None, :]).astype(jnp.float32)
    picked = jnp.sum(picked_mask * scores[:, None, :], axis=-1)
    chosen = jnp.sum(picked_mask, axis=1)
    combine = chosen * scores * ROUTE_SCALE / jnp.sum(picked, axis=-1, keepdims=True)
    held_weights = combine[:, : w_gate.shape[0]]
    full_gate, full_up, full_down = (
        lax.all_gather(w_gate, "dp", axis=1, tiled=True),
        lax.all_gather(w_up, "dp", axis=1, tiled=True),
        lax.all_gather(w_down, "dp", axis=1, tiled=True),
    )
    gate_value = jnp.einsum("td,edf->tef", normed, full_gate, preferred_element_type=jnp.float32)
    up_value = jnp.einsum("td,edf->tef", normed, full_up, preferred_element_type=jnp.float32)
    hidden = (jax.nn.silu(gate_value) * up_value * held_weights[:, :, None]).astype(jnp.bfloat16)
    whole_hidden = lax.all_gather(hidden, "tp", axis=2, tiled=True)
    mixed = jnp.einsum("tef,efd->td", whole_hidden, full_down, preferred_element_type=jnp.float32)
    return mixed.astype(jnp.bfloat16)


def kernel(
    groups, tps, x_hbm, gain_ref, router_ref, routes_ref, wg_hbm, wu_hbm, wd_hbm, o_ref,
    x, w, dn, hid, comb,
    x_sem, own_sem, recv_sem, up_sem, down_sem, side_sem, hid_send, hid_recv,
):
    dp, tp = lax.axis_index("dp"), lax.axis_index("tp")
    positions = groups // CORES
    z, core = dp // CORES, dp % CORES
    experts = wg_hbm.shape[0]
    rows = x.shape[0]
    top, bottom = z == positions - 1, z == 0
    above = (jnp.minimum(z + 1, positions - 1) * CORES + core, tp)
    below = (jnp.maximum(z - 1, 0) * CORES + core, tp)
    side = (z * CORES + (1 - core), tp)

    load_x = pltpu.make_async_copy(x_hbm, x, x_sem)
    load_x.start()
    chunks = [(m, e) for e in range(experts) for m in (0, 1)] + [(2, e) for e in range(experts)]

    def source(k):
        m, e = chunks[k]
        return (wg_hbm, wu_hbm, wd_hbm)[m].at[e]

    def slot(k, d):
        m, e = chunks[k]
        return dn.at[e, d] if m == 2 else w.at[m, e, d]

    def copy_own(k):
        return pltpu.make_async_copy(source(k), slot(k, dp), own_sem.at[k])

    for k in range(len(chunks)):
        copy_own(k).start()

    barrier = pltpu.get_barrier_semaphore()
    pl.semaphore_signal(barrier, inc=1, device_id=side, device_id_type=MESH)
    for i in range(1, tps):
        pl.semaphore_signal(
            barrier, inc=1, device_id=(dp, lax.rem(tp + i, tps)), device_id_type=MESH
        )

    @pl.when(jnp.logical_not(top))
    def _():
        pl.semaphore_signal(barrier, inc=1, device_id=above, device_id_type=MESH)

    @pl.when(jnp.logical_not(bottom))
    def _():
        pl.semaphore_signal(barrier, inc=1, device_id=below, device_id_type=MESH)

    ends = jnp.where(top, 1, 0) + jnp.where(bottom, 1, 0)
    pl.semaphore_wait(barrier, tps + 2 - ends)

    def send(k, d, src, sem, to):
        return pltpu.make_async_remote_copy(
            src_ref=src, dst_ref=slot(k, d), send_sem=sem.at[k, d // CORES],
            recv_sem=recv_sem.at[k, d], device_id=to, device_id_type=MESH,
        )

    def arrived(k, d):
        pltpu.make_async_remote_copy(
            src_ref=slot(k, d), dst_ref=slot(k, d), send_sem=side_sem.at[k, d // CORES],
            recv_sem=recv_sem.at[k, d], device_id=side, device_id_type=MESH,
        ).wait_recv()

    def send_own(k):
        @pl.when(jnp.logical_not(top))
        def _():
            send(k, dp, source(k), up_sem, above).start()

        @pl.when(jnp.logical_not(bottom))
        def _():
            send(k, dp, source(k), down_sem, below).start()

        send(k, dp, source(k), side_sem, side).start()

    def relay(k):
        for j in range(1, positions):
            @pl.when(z - j >= 0)
            def _():
                d = dp - j * CORES
                arrived(k, d)

                @pl.when(jnp.logical_not(top))
                def _():
                    send(k, d, slot(k, d), up_sem, above).start()

                send(k, d, slot(k, d), side_sem, side).start()

            @pl.when(z + j <= positions - 1)
            def _():
                d = dp + j * CORES
                arrived(k, d)

                @pl.when(jnp.logical_not(bottom))
                def _():
                    send(k, d, slot(k, d), down_sem, below).start()

                send(k, d, slot(k, d), side_sem, side).start()

    def wait_side(k):
        for p in range(positions):
            arrived(k, p * CORES + (1 - core))
        copy_own(k).wait()

    def norm():
        step = rows // 8

        def body(i, _):
            part = pl.ds(pl.multiple_of(i * step, step), step)
            v = x[part, :].astype(jnp.float32)
            square = jnp.mean(v * v, axis=-1, keepdims=True)
            x[part, :] = (v * lax.rsqrt(square + EPS) * gain_ref[...]).astype(jnp.bfloat16)
            return 0

        lax.fori_loop(0, 8, body, 0)

    def score():
        rest = router_ref[...]
        total = jnp.zeros((rows, rest.shape[0]), jnp.float32)
        parts = []
        for _ in range(3):
            part = rest.astype(jnp.bfloat16)
            rest = rest - part.astype(jnp.float32)
            parts.append(part)
        for part in parts[::-1]:
            total += lax.dot_general(
                x[...], part, (((1,), (1,)), ((), ())), preferred_element_type=jnp.float32
            )
        scores = 1.0 / (1.0 + jnp.exp(-total))
        routed = scores.shape[1]
        picks = routes_ref[...].astype(jnp.float32)
        labels = lax.broadcasted_iota(jnp.int32, scores.shape, 1).astype(jnp.float32)
        chosen = jnp.zeros_like(scores)
        for i in range(routes_ref.shape[0]):
            column = jnp.transpose(jnp.broadcast_to(picks[i : i + 1, :], (128, rows)))
            chosen += jnp.where(column[:, :routed] == labels, 1.0, 0.0)
        picked = chosen * scores
        comb[...] = picked * ROUTE_SCALE / jnp.sum(picked, axis=-1, keepdims=True)

    def send_hidden(e, i):
        return pltpu.make_async_remote_copy(
            src_ref=hid.at[e, tp], dst_ref=hid.at[e, tp], send_sem=hid_send.at[e, i - 1],
            recv_sem=hid_recv.at[e, tp],
            device_id=(dp, lax.rem(tp + i, tps)), device_id_type=MESH,
        )

    def experts_hidden(e):
        step = rows // 2

        def body(i, _):
            part = pl.ds(pl.multiple_of(i * step, step), step)
            lhs = x[part, :]
            depth = x.shape[1]
            gate = jnp.dot(
                lhs, w[0, e].reshape(depth, w.shape[-1]), preferred_element_type=jnp.float32
            )
            up = jnp.dot(
                lhs, w[1, e].reshape(depth, w.shape[-1]), preferred_element_type=jnp.float32
            )
            hid[e, tp, part, :] = (gate / (1.0 + jnp.exp(-gate)) * up).astype(jnp.bfloat16)
            return 0

        lax.fori_loop(0, 2, body, 0)
        for i in range(1, tps):
            send_hidden(e, i).start()

    def down():
        cols = o_ref.shape[1]
        step = cols // 4

        def body(i, _):
            part = pl.ds(pl.multiple_of(i * step, step), step)
            total = None
            for e in range(experts):
                lhs = jnp.concatenate([hid[e, t] for t in range(tps)], axis=1)
                rhs = dn[e, :, :, part].reshape(lhs.shape[1], step)
                term = jnp.dot(lhs, rhs, preferred_element_type=jnp.float32)
                term = term * comb[:, e : e + 1]
                total = term if total is None else total + term
            o_ref[:, part] = total.astype(o_ref.dtype)
            return 0

        lax.fori_loop(0, 4, body, 0)

    ahead = 2
    for k in range(min(ahead, len(chunks))):
        send_own(k)
    for k in range(len(chunks)):
        relay(k)
        if k + ahead < len(chunks):
            send_own(k + ahead)
        m, e = chunks[k]
        if k == 0:
            load_x.wait()
            norm()
        if k == 2:
            score()
        if m == 1:
            wait_side(k - 1)
            wait_side(k)
            experts_hidden(e)
    for k, (m, e) in enumerate(chunks):
        if m == 2:
            wait_side(k)
    for e in range(experts):
        for i in range(1, tps):
            s = lax.rem(tp + i, tps)
            pltpu.make_async_remote_copy(
                src_ref=hid.at[e, s], dst_ref=hid.at[e, s], send_sem=hid_send.at[e, i - 1],
                recv_sem=hid_recv.at[e, s], device_id=side, device_id_type=MESH,
            ).wait_recv()
    down()

    for e in range(experts):
        for i in range(1, tps):
            send_hidden(e, i).wait_send()
    for k in range(len(chunks)):
        for p in range(positions):
            d = p * CORES + core
            send(k, d, slot(k, d), side_sem, side).wait_send()

            @pl.when(jnp.logical_and(jnp.logical_not(top), p <= z))
            def _():
                send(k, d, slot(k, d), up_sem, above).wait_send()

            @pl.when(jnp.logical_and(jnp.logical_not(bottom), p >= z))
            def _():
                send(k, d, slot(k, d), down_sem, below).wait_send()


def streamed(groups, tps, tokens, gain, router, routes, w_gate, w_up, w_down):
    rows, depth = tokens.shape
    experts, shard, width = w_gate.shape
    down_rows, cols = w_down.shape[1:]
    positions = groups // CORES
    vmem = pl.BlockSpec(memory_space=pltpu.VMEM)
    hbm = pl.BlockSpec(memory_space=pl.ANY)
    chunks = 3 * experts
    dma = pltpu.SemaphoreType.DMA
    return pl.pallas_call(
        functools.partial(kernel, groups, tps),
        out_shape=jax.ShapeDtypeStruct((rows, cols), jnp.bfloat16),
        in_specs=[hbm, vmem, vmem, vmem, hbm, hbm, hbm],
        out_specs=vmem,
        scratch_shapes=[
            pltpu.VMEM((rows, depth), jnp.bfloat16),
            pltpu.VMEM((2, experts, groups, shard, width), jnp.bfloat16),
            pltpu.VMEM((experts, groups, down_rows, cols), jnp.bfloat16),
            pltpu.VMEM((experts, tps, rows, width), jnp.bfloat16),
            pltpu.VMEM((rows, router.shape[1]), jnp.float32),
            dma,
            dma((chunks,)),
            dma((chunks, groups)),
            dma((chunks, positions)),
            dma((chunks, positions)),
            dma((chunks, positions)),
            dma((experts, tps - 1)),
            dma((experts, tps)),
        ],
        compiler_params=pltpu.CompilerParams(
            collective_id=0, has_side_effects=True, vmem_limit_bytes=60 * 1024 * 1024
        ),
    )(tokens, gain.reshape(1, -1), router.T, routes.T, w_gate, w_up, w_down)


def solution(mesh):
    groups, tps = mesh.shape["dp"], mesh.shape["tp"]
    fits = groups % CORES == 0 and groups // CORES <= 4
    body = functools.partial(streamed, groups, tps) if fits else gathered
    return jax.shard_map(
        body,
        mesh=mesh,
        in_specs=(
            P("dp", None),
            P(),
            P(),
            P("dp", None),
            P(None, "dp", "tp"),
            P(None, "dp", "tp"),
            P(None, "dp", "tp"),
        ),
        out_specs=P("dp", "tp"),
        check_vma=False,
    )
```

```python
import functools

import jax
import jax.numpy as jnp
from jax import lax
from jax.experimental import pallas as pl
from jax.experimental.pallas import tpu as pltpu
from jax.sharding import PartitionSpec as P

EPS = 1e-06
ROUTE_SCALE = 2.5
MESH = pl.DeviceIdType.MESH
CORES = 2
PIECES = 4
HOSTED = (0,)


def gathered(tokens, gain, router, routes, w_gate, w_up, w_down):
    values = tokens.astype(jnp.float32)
    square = jnp.mean(values * values, axis=-1, keepdims=True)
    normed = (values * lax.rsqrt(square + EPS) * gain).astype(jnp.bfloat16)
    scores = jax.nn.sigmoid(
        jnp.dot(normed.astype(jnp.float32), router, precision=lax.Precision.HIGHEST)
    )
    labels = jnp.arange(router.shape[1], dtype=jnp.int32)
    picked_mask = (routes[:, :, None] == labels[None, None, :]).astype(jnp.float32)
    picked = jnp.sum(picked_mask * scores[:, None, :], axis=-1)
    chosen = jnp.sum(picked_mask, axis=1)
    combine = chosen * scores * ROUTE_SCALE / jnp.sum(picked, axis=-1, keepdims=True)
    held_weights = combine[:, : w_gate.shape[0]]
    full_gate, full_up, full_down = (
        lax.all_gather(w_gate, "dp", axis=1, tiled=True),
        lax.all_gather(w_up, "dp", axis=1, tiled=True),
        lax.all_gather(w_down, "dp", axis=1, tiled=True),
    )
    gate_value = jnp.einsum("td,edf->tef", normed, full_gate, preferred_element_type=jnp.float32)
    up_value = jnp.einsum("td,edf->tef", normed, full_up, preferred_element_type=jnp.float32)
    hidden = (jax.nn.silu(gate_value) * up_value * held_weights[:, :, None]).astype(jnp.bfloat16)
    whole_hidden = lax.all_gather(hidden, "tp", axis=2, tiled=True)
    mixed = jnp.einsum("tef,efd->td", whole_hidden, full_down, preferred_element_type=jnp.float32)
    return mixed.astype(jnp.bfloat16)


def kernel(
    groups, tps, hosted, x_hbm, gain_ref, router_ref, routes_ref, wg_hbm, wu_hbm, wd_hbm, o_ref,
    x, guest, guest_normed, w, dn, hid, guest_hid, comb,
    x_sem, own_sem, recv_sem, in_sem, out_sem, side_sem, hid_send, hid_recv,
    tok_send, tok_recv, back_send, back_recv,
):
    dp, tp = lax.axis_index("dp"), lax.axis_index("tp")
    positions = groups // CORES
    z, core = dp // CORES, dp % CORES
    experts = wg_hbm.shape[0]
    rows = x.shape[0]
    end = jnp.logical_or(z == positions - 1, z == 0)
    out = 2 * (2 * z // positions) - 1

    def at(p):
        return (p * CORES + core, tp)

    inner = at(z - out)
    outer = at(jnp.clip(z + out, 0, positions - 1))
    side = (z * CORES + (1 - core), tp)
    along_x = tp + 1 - 2 * (tp % 2)
    along_y = lax.rem(tp + 2, tps)
    across = lax.rem(along_x + 2, tps)

    load_x = pltpu.make_async_copy(x_hbm, x, x_sem)
    load_x.start()
    order = sorted(range(experts), key=lambda e: e not in hosted)
    chunks = [(m, e) for e in order for m in (0, 1)] + [(2, e) for e in range(experts)]
    everywhere = [k for k, (m, e) in enumerate(chunks) if m == 2 or e not in hosted]
    feeds = [k for k, (m, e) in enumerate(chunks) if m < 2]
    downs = [k for k, (m, e) in enumerate(chunks) if m == 2]

    def source(k):
        m, e = chunks[k]
        return (wg_hbm, wu_hbm, wd_hbm)[m].at[e]

    def slot(k, d):
        m, e = chunks[k]
        return dn.at[e, d] if m == 2 else w.at[m, e, d]

    def copy_own(k):
        return pltpu.make_async_copy(source(k), slot(k, dp), own_sem.at[k])

    for k in range(len(chunks)):
        copy_own(k).start()

    barrier = pltpu.get_barrier_semaphore()
    pl.semaphore_signal(barrier, inc=1, device_id=side, device_id_type=MESH)
    pl.semaphore_signal(barrier, inc=1, device_id=inner, device_id_type=MESH)
    for i in range(1, tps):
        pl.semaphore_signal(
            barrier, inc=1, device_id=(dp, lax.rem(tp + i, tps)), device_id_type=MESH
        )

    @pl.when(jnp.logical_not(end))
    def _():
        pl.semaphore_signal(barrier, inc=1, device_id=outer, device_id_type=MESH)

    pl.semaphore_wait(barrier, tps + 2 - jnp.where(end, 1, 0))

    def send(k, d, src, sem, to):
        return pltpu.make_async_remote_copy(
            src_ref=src, dst_ref=slot(k, d), send_sem=sem.at[k, d // CORES],
            recv_sem=recv_sem.at[k, d], device_id=to, device_id_type=MESH,
        )

    def arrived(k, d):
        send(k, d, slot(k, d), side_sem, side).wait_recv()

    def pass_on(k, p, targets):
        d = p * CORES + core
        arrived(k, d)
        for sem, to in targets:
            send(k, d, slot(k, d), sem, to).start()

    def wait_side(k):
        for p in range(positions):
            arrived(k, p * CORES + (1 - core))
        copy_own(k).wait()

    quarter = rows // tps
    piece = quarter // PIECES

    def token_part(q, p):
        return pl.ds(pl.multiple_of(q * quarter + p * piece, piece), piece)

    def token_copy(src, q, p, kind, to):
        return pltpu.make_async_remote_copy(
            src_ref=src.at[token_part(q, p)], dst_ref=guest.at[token_part(q, p)],
            send_sem=tok_send.at[kind, p], recv_sem=tok_recv.at[q, p],
            device_id=to, device_id_type=MESH,
        )

    def token_arrived(q, p):
        token_copy(guest, q, p, 0, side).wait_recv()

    def norm(src, dst, start, count, steps):
        step = count // steps

        def body(i, _):
            part = pl.ds(pl.multiple_of(start + i * step, step), step)
            v = src[part, :].astype(jnp.float32)
            square = jnp.mean(v * v, axis=-1, keepdims=True)
            dst[part, :] = (v * lax.rsqrt(square + EPS) * gain_ref[...]).astype(jnp.bfloat16)
            return 0

        lax.fori_loop(0, steps, body, 0)

    def norm_quarter(q):
        norm(guest, guest_normed, q * quarter, quarter, 2)

    def score():
        rest = router_ref[...]
        total = jnp.zeros((rows, rest.shape[0]), jnp.float32)
        parts = []
        for _ in range(3):
            part = rest.astype(jnp.bfloat16)
            rest = rest - part.astype(jnp.float32)
            parts.append(part)
        for part in parts[::-1]:
            total += lax.dot_general(
                x[...], part, (((1,), (1,)), ((), ())), preferred_element_type=jnp.float32
            )
        scores = 1.0 / (1.0 + jnp.exp(-total))
        routed = scores.shape[1]
        picks = routes_ref[...].astype(jnp.float32)
        labels = lax.broadcasted_iota(jnp.int32, scores.shape, 1).astype(jnp.float32)
        chosen = jnp.zeros_like(scores)
        for i in range(routes_ref.shape[0]):
            column = jnp.transpose(jnp.broadcast_to(picks[i : i + 1, :], (128, rows)))
            chosen += jnp.where(column[:, :routed] == labels, 1.0, 0.0)
        picked = chosen * scores
        comb[...] = picked * ROUTE_SCALE / jnp.sum(picked, axis=-1, keepdims=True)

    def send_hidden(e, i):
        return pltpu.make_async_remote_copy(
            src_ref=hid.at[e, tp], dst_ref=hid.at[e, tp], send_sem=hid_send.at[e, i - 1],
            recv_sem=hid_recv.at[e, tp],
            device_id=(dp, lax.rem(tp + i, tps)), device_id_type=MESH,
        )

    def share_hidden(e):
        for i in range(1, tps):
            send_hidden(e, i).start()

    def send_back(e):
        return pltpu.make_async_remote_copy(
            src_ref=guest_hid.at[e], dst_ref=hid.at[e, tp], send_sem=back_send.at[e],
            recv_sem=back_recv.at[e], device_id=outer, device_id_type=MESH,
        )

    def expert_hidden(e, src, dst):
        step = rows // 2

        def body(i, _):
            part = pl.ds(pl.multiple_of(i * step, step), step)
            lhs = src[part, :]
            depth = x.shape[1]
            gate = jnp.dot(
                lhs, w[0, e].reshape(depth, w.shape[-1]), preferred_element_type=jnp.float32
            )
            up = jnp.dot(
                lhs, w[1, e].reshape(depth, w.shape[-1]), preferred_element_type=jnp.float32
            )
            dst[part, :] = (gate / (1.0 + jnp.exp(-gate)) * up).astype(jnp.bfloat16)
            return 0

        lax.fori_loop(0, 2, body, 0)

    def own_hidden(e):
        expert_hidden(e, x, hid.at[e, tp])
        share_hidden(e)

    def guest_hidden(e):
        expert_hidden(e, guest_normed, guest_hid.at[e])
        send_back(e).start()

    def sides_of(e):
        for k in feeds:
            if chunks[k][1] == e:
                wait_side(k)

    def down():
        cols = o_ref.shape[1]
        step = cols // 4

        def body(i, _):
            part = pl.ds(pl.multiple_of(i * step, step), step)
            total = None
            for e in range(experts):
                lhs = jnp.concatenate([hid[e, t] for t in range(tps)], axis=1)
                rhs = dn[e, :, :, part].reshape(lhs.shape[1], step)
                term = jnp.dot(lhs, rhs, preferred_element_type=jnp.float32)
                term = term * comb[:, e : e + 1]
                total = term if total is None else total + term
            o_ref[:, part] = total.astype(o_ref.dtype)
            return 0

        lax.fori_loop(0, 4, body, 0)

    to_in, to_out, to_side = (in_sem, inner), (out_sem, outer), (side_sem, side)

    @pl.when(end)
    def _():
        for p in range(PIECES):
            token_copy(x_hbm, tp, p, 0, inner).start()
        for k in range(len(chunks)):
            send(k, dp, source(k), *to_in).start()
        for k in everywhere:
            send(k, dp, source(k), *to_side).start()
        load_x.wait()
        norm(x, x, 0, rows, 8)
        score()
        for j in range(1, positions - 1):
            for k in everywhere:
                pass_on(k, z - j * out, [to_side])
        for e in order:
            if e in hosted:
                send_back(e).wait_recv()
                share_hidden(e)
        for e in order:
            if e not in hosted:
                for k in feeds:
                    if chunks[k][1] == e:
                        pass_on(k, z - (positions - 1) * out, [to_side])
                sides_of(e)
                own_hidden(e)
        for k in downs:
            pass_on(k, z - (positions - 1) * out, [to_side])
        for k in range(len(chunks)):
            if k not in everywhere:
                copy_own(k).wait()

    @pl.when(jnp.logical_not(end))
    def _():
        def beyond(k):
            return [to_out] if k in everywhere else []

        for k in range(len(chunks)):
            send(k, dp, source(k), *to_in).start()
        for k in everywhere:
            send(k, dp, source(k), *to_out).start()
        for k in range(len(chunks)):
            send(k, dp, source(k), *to_side).start()

        def from_outer(k):
            pass_on(k, z + out, [to_in, to_side])

        def from_near(k):
            pass_on(k, z - out, beyond(k) + [to_side])

        def from_far(k):
            pass_on(k, z - 2 * out, beyond(k) + [to_side])

        load_x.wait()
        norm(x, x, 0, rows, 8)
        for p in range(PIECES):
            token_arrived(tp, p)
            token_copy(guest, tp, p, 0, (dp, along_x)).start()
            token_copy(guest, tp, p, 1, (dp, along_y)).start()
            from_near(p)
        norm_quarter(tp)
        for p in range(PIECES):
            token_arrived(along_x, p)
            if p < PIECES // 2:
                token_copy(guest, along_x, p, 2, (dp, along_y)).start()
            token_arrived(along_y, p)
            if p >= PIECES // 2:
                token_copy(guest, along_y, p, 2, (dp, along_x)).start()
            if p == 1:
                score()
                for k in downs:
                    from_near(k)
            if p == 2:
                from_outer(feeds[0])
        from_outer(feeds[1])
        norm_quarter(along_x)
        norm_quarter(along_y)
        from_far(feeds[0])
        from_outer(feeds[2])
        for p in range(PIECES):
            token_arrived(across, p)
        norm_quarter(across)
        from_far(feeds[1])
        from_outer(feeds[3])
        sides_of(order[0])
        guest_hidden(order[0])
        from_outer(downs[0])
        from_far(feeds[2])
        own_hidden(order[0])
        from_outer(downs[1])
        from_far(feeds[3])
        sides_of(order[1])
        if order[1] in hosted:
            guest_hidden(order[1])
        own_hidden(order[1])
        for k in downs:
            from_far(k)

    for k in downs:
        wait_side(k)
    for e in order:
        for i in range(1, tps):
            s = lax.rem(tp + i, tps)
            pltpu.make_async_remote_copy(
                src_ref=hid.at[e, s], dst_ref=hid.at[e, s], send_sem=hid_send.at[e, i - 1],
                recv_sem=hid_recv.at[e, s], device_id=side, device_id_type=MESH,
            ).wait_recv()
    down()

    def sent(k, p, sem):
        d = p * CORES + core
        send(k, d, slot(k, d), sem, side).wait_send()

    for e in range(experts):
        for i in range(1, tps):
            send_hidden(e, i).wait_send()
    for k in range(len(chunks)):
        sent(k, z, in_sem)

    @pl.when(end)
    def _():
        for p in range(PIECES):
            token_copy(x_hbm, tp, p, 0, inner).wait_send()
        for k in everywhere:
            for p in range(positions):
                sent(k, p, side_sem)

    @pl.when(jnp.logical_not(end))
    def _():
        for p in range(PIECES):
            for kind in range(3):
                token_copy(guest, tp, p, kind, side).wait_send()
        for e in hosted:
            send_back(e).wait_send()
        for k in range(len(chunks)):
            sent(k, z + out, in_sem)
            for p in range(positions):
                sent(k, p, side_sem)
        for k in everywhere:
            sent(k, z, out_sem)
            sent(k, z - out, out_sem)
            sent(k, z - 2 * out, out_sem)


def streamed(groups, tps, tokens, gain, router, routes, w_gate, w_up, w_down):
    rows, depth = tokens.shape
    experts, shard, width = w_gate.shape
    down_rows, cols = w_down.shape[1:]
    positions = groups // CORES
    vmem = pl.BlockSpec(memory_space=pltpu.VMEM)
    hbm = pl.BlockSpec(memory_space=pl.ANY)
    chunks = 3 * experts
    dma = pltpu.SemaphoreType.DMA
    return pl.pallas_call(
        functools.partial(kernel, groups, tps, HOSTED),
        out_shape=jax.ShapeDtypeStruct((rows, cols), jnp.bfloat16),
        in_specs=[hbm, vmem, vmem, vmem, hbm, hbm, hbm],
        out_specs=vmem,
        scratch_shapes=[
            pltpu.VMEM((rows, depth), jnp.bfloat16),
            pltpu.VMEM((rows, depth), jnp.bfloat16),
            pltpu.VMEM((rows, depth), jnp.bfloat16),
            pltpu.VMEM((2, experts, groups, shard, width), jnp.bfloat16),
            pltpu.VMEM((experts, groups, down_rows, cols), jnp.bfloat16),
            pltpu.VMEM((experts, tps, rows, width), jnp.bfloat16),
            pltpu.VMEM((experts, rows, width), jnp.bfloat16),
            pltpu.VMEM((rows, router.shape[1]), jnp.float32),
            dma,
            dma((chunks,)),
            dma((chunks, groups)),
            dma((chunks, positions)),
            dma((chunks, positions)),
            dma((chunks, positions)),
            dma((experts, tps - 1)),
            dma((experts, tps)),
            dma((3, PIECES)),
            dma((tps, PIECES)),
            dma((experts,)),
            dma((experts,)),
        ],
        compiler_params=pltpu.CompilerParams(
            collective_id=0, has_side_effects=True, vmem_limit_bytes=60 * 1024 * 1024
        ),
    )(tokens, gain.reshape(1, -1), router.T, routes.T, w_gate, w_up, w_down)


def solution(mesh):
    groups, tps = mesh.shape["dp"], mesh.shape["tp"]
    fits = groups == 4 * CORES and tps == 4
    body = functools.partial(streamed, groups, tps) if fits else gathered
    return jax.shard_map(
        body,
        mesh=mesh,
        in_specs=(
            P("dp", None),
            P(),
            P(),
            P("dp", None),
            P(None, "dp", "tp"),
            P(None, "dp", "tp"),
            P(None, "dp", "tp"),
        ),
        out_specs=P("dp", "tp"),
        check_vma=False,
    )
```

```python
import functools

import jax
import jax.numpy as jnp
from jax import lax
from jax.experimental import pallas as pl
from jax.experimental.pallas import tpu as pltpu
from jax.sharding import PartitionSpec as P

EPS = 1e-06
ROUTE_SCALE = 2.5
MESH = pl.DeviceIdType.MESH
CORES = 2
PIECES = 4
HOSTED = (0, 1)


def gathered(tokens, gain, router, routes, w_gate, w_up, w_down):
    values = tokens.astype(jnp.float32)
    square = jnp.mean(values * values, axis=-1, keepdims=True)
    normed = (values * lax.rsqrt(square + EPS) * gain).astype(jnp.bfloat16)
    scores = jax.nn.sigmoid(
        jnp.dot(normed.astype(jnp.float32), router, precision=lax.Precision.HIGHEST)
    )
    labels = jnp.arange(router.shape[1], dtype=jnp.int32)
    picked_mask = (routes[:, :, None] == labels[None, None, :]).astype(jnp.float32)
    picked = jnp.sum(picked_mask * scores[:, None, :], axis=-1)
    chosen = jnp.sum(picked_mask, axis=1)
    combine = chosen * scores * ROUTE_SCALE / jnp.sum(picked, axis=-1, keepdims=True)
    held_weights = combine[:, : w_gate.shape[0]]
    full_gate, full_up, full_down = (
        lax.all_gather(w_gate, "dp", axis=1, tiled=True),
        lax.all_gather(w_up, "dp", axis=1, tiled=True),
        lax.all_gather(w_down, "dp", axis=1, tiled=True),
    )
    gate_value = jnp.einsum("td,edf->tef", normed, full_gate, preferred_element_type=jnp.float32)
    up_value = jnp.einsum("td,edf->tef", normed, full_up, preferred_element_type=jnp.float32)
    hidden = (jax.nn.silu(gate_value) * up_value * held_weights[:, :, None]).astype(jnp.bfloat16)
    whole_hidden = lax.all_gather(hidden, "tp", axis=2, tiled=True)
    mixed = jnp.einsum("tef,efd->td", whole_hidden, full_down, preferred_element_type=jnp.float32)
    return mixed.astype(jnp.bfloat16)


def kernel(
    groups, tps, hosted, x_hbm, gain_ref, router_ref, routes_ref, wg_hbm, wu_hbm, wd_hbm, o_ref,
    x, guest, guest_normed, w, dn, hid, guest_hid, comb,
    x_sem, own_sem, recv_sem, in_sem, out_sem, side_sem, hid_send, hid_recv,
    tok_send, tok_recv, back_send, back_recv,
):
    dp, tp = lax.axis_index("dp"), lax.axis_index("tp")
    positions = groups // CORES
    z, core = dp // CORES, dp % CORES
    experts = wg_hbm.shape[0]
    rows = x.shape[0]
    end = jnp.logical_or(z == positions - 1, z == 0)
    out = 2 * (2 * z // positions) - 1

    def at(p):
        return (p * CORES + core, tp)

    inner = at(z - out)
    outer = at(jnp.clip(z + out, 0, positions - 1))
    side = (z * CORES + (1 - core), tp)
    along_x = tp + 1 - 2 * (tp % 2)
    along_y = lax.rem(tp + 2, tps)
    across = lax.rem(along_x + 2, tps)

    load_x = pltpu.make_async_copy(x_hbm, x, x_sem)
    load_x.start()
    order = sorted(range(experts), key=lambda e: e not in hosted)
    chunks = [(m, e) for e in order for m in (0, 1)] + [(2, e) for e in range(experts)]
    everywhere = [k for k, (m, e) in enumerate(chunks) if m == 2 or e not in hosted]
    feeds = [k for k, (m, e) in enumerate(chunks) if m < 2]
    downs = [k for k, (m, e) in enumerate(chunks) if m == 2]

    def source(k):
        m, e = chunks[k]
        return (wg_hbm, wu_hbm, wd_hbm)[m].at[e]

    def slot(k, d):
        m, e = chunks[k]
        return dn.at[e, d] if m == 2 else w.at[m, e, d]

    def copy_own(k):
        return pltpu.make_async_copy(source(k), slot(k, dp), own_sem.at[k])

    for k in range(len(chunks)):
        copy_own(k).start()

    barrier = pltpu.get_barrier_semaphore()
    pl.semaphore_signal(barrier, inc=1, device_id=side, device_id_type=MESH)
    pl.semaphore_signal(barrier, inc=1, device_id=inner, device_id_type=MESH)
    for i in range(1, tps):
        pl.semaphore_signal(
            barrier, inc=1, device_id=(dp, lax.rem(tp + i, tps)), device_id_type=MESH
        )

    @pl.when(jnp.logical_not(end))
    def _():
        pl.semaphore_signal(barrier, inc=1, device_id=outer, device_id_type=MESH)

    pl.semaphore_wait(barrier, tps + 2 - jnp.where(end, 1, 0))

    def send(k, d, src, sem, to):
        return pltpu.make_async_remote_copy(
            src_ref=src, dst_ref=slot(k, d), send_sem=sem.at[k, d // CORES],
            recv_sem=recv_sem.at[k, d], device_id=to, device_id_type=MESH,
        )

    def arrived(k, d):
        send(k, d, slot(k, d), side_sem, side).wait_recv()

    def pass_on(k, p, targets):
        d = p * CORES + core
        arrived(k, d)
        for sem, to in targets:
            send(k, d, slot(k, d), sem, to).start()

    def wait_side(k):
        for p in range(positions):
            arrived(k, p * CORES + (1 - core))
        copy_own(k).wait()

    quarter = rows // tps
    piece = quarter // PIECES

    def token_part(q, p):
        return pl.ds(pl.multiple_of(q * quarter + p * piece, piece), piece)

    def token_copy(src, q, p, kind, to):
        return pltpu.make_async_remote_copy(
            src_ref=src.at[token_part(q, p)], dst_ref=guest.at[token_part(q, p)],
            send_sem=tok_send.at[kind, p], recv_sem=tok_recv.at[q, p],
            device_id=to, device_id_type=MESH,
        )

    def token_arrived(q, p):
        token_copy(guest, q, p, 0, side).wait_recv()

    def norm(src, dst, start, count, steps):
        step = count // steps

        def body(i, _):
            part = pl.ds(pl.multiple_of(start + i * step, step), step)
            v = src[part, :].astype(jnp.float32)
            square = jnp.mean(v * v, axis=-1, keepdims=True)
            dst[part, :] = (v * lax.rsqrt(square + EPS) * gain_ref[...]).astype(jnp.bfloat16)
            return 0

        lax.fori_loop(0, steps, body, 0)

    def norm_quarter(q):
        norm(guest, guest_normed, q * quarter, quarter, 2)

    def score():
        rest = router_ref[...]
        total = jnp.zeros((rows, rest.shape[0]), jnp.float32)
        parts = []
        for _ in range(3):
            part = rest.astype(jnp.bfloat16)
            rest = rest - part.astype(jnp.float32)
            parts.append(part)
        for part in parts[::-1]:
            total += lax.dot_general(
                x[...], part, (((1,), (1,)), ((), ())), preferred_element_type=jnp.float32
            )
        scores = 1.0 / (1.0 + jnp.exp(-total))
        routed = scores.shape[1]
        picks = routes_ref[...].astype(jnp.float32)
        labels = lax.broadcasted_iota(jnp.int32, scores.shape, 1).astype(jnp.float32)
        chosen = jnp.zeros_like(scores)
        for i in range(routes_ref.shape[0]):
            column = jnp.transpose(jnp.broadcast_to(picks[i : i + 1, :], (128, rows)))
            chosen += jnp.where(column[:, :routed] == labels, 1.0, 0.0)
        picked = chosen * scores
        comb[...] = picked * ROUTE_SCALE / jnp.sum(picked, axis=-1, keepdims=True)

    def send_hidden(e, i):
        return pltpu.make_async_remote_copy(
            src_ref=hid.at[e, tp], dst_ref=hid.at[e, tp], send_sem=hid_send.at[e, i - 1],
            recv_sem=hid_recv.at[e, tp],
            device_id=(dp, lax.rem(tp + i, tps)), device_id_type=MESH,
        )

    def share_hidden(e):
        for i in range(1, tps):
            send_hidden(e, i).start()

    def send_back(e):
        return pltpu.make_async_remote_copy(
            src_ref=guest_hid.at[e], dst_ref=hid.at[e, tp], send_sem=back_send.at[e],
            recv_sem=back_recv.at[e], device_id=outer, device_id_type=MESH,
        )

    def expert_hidden(e, src, dst):
        step = rows // 2

        def body(i, _):
            part = pl.ds(pl.multiple_of(i * step, step), step)
            lhs = src[part, :]
            depth = x.shape[1]
            gate = jnp.dot(
                lhs, w[0, e].reshape(depth, w.shape[-1]), preferred_element_type=jnp.float32
            )
            up = jnp.dot(
                lhs, w[1, e].reshape(depth, w.shape[-1]), preferred_element_type=jnp.float32
            )
            dst[part, :] = (gate / (1.0 + jnp.exp(-gate)) * up).astype(jnp.bfloat16)
            return 0

        lax.fori_loop(0, 2, body, 0)

    def own_hidden(e):
        expert_hidden(e, x, hid.at[e, tp])
        share_hidden(e)

    def guest_hidden(e):
        expert_hidden(e, guest_normed, guest_hid.at[e])
        send_back(e).start()

    def sides_of(e):
        for k in feeds:
            if chunks[k][1] == e:
                wait_side(k)

    def down():
        cols = o_ref.shape[1]
        step = cols // 4

        def body(i, _):
            part = pl.ds(pl.multiple_of(i * step, step), step)
            total = None
            for e in range(experts):
                lhs = jnp.concatenate([hid[e, t] for t in range(tps)], axis=1)
                rhs = dn[e, :, :, part].reshape(lhs.shape[1], step)
                term = jnp.dot(lhs, rhs, preferred_element_type=jnp.float32)
                term = term * comb[:, e : e + 1]
                total = term if total is None else total + term
            o_ref[:, part] = total.astype(o_ref.dtype)
            return 0

        lax.fori_loop(0, 4, body, 0)

    to_in, to_out, to_side = (in_sem, inner), (out_sem, outer), (side_sem, side)

    @pl.when(end)
    def _():
        for p in range(PIECES):
            token_copy(x_hbm, tp, p, 0, inner).start()
        for k in range(len(chunks)):
            send(k, dp, source(k), *to_in).start()
        for k in everywhere:
            send(k, dp, source(k), *to_side).start()
        load_x.wait()
        norm(x, x, 0, rows, 8)
        score()
        for j in range(1, positions - 1):
            for k in everywhere:
                pass_on(k, z - j * out, [to_side])
        for e in order:
            if e in hosted:
                send_back(e).wait_recv()
                share_hidden(e)
        for e in order:
            if e not in hosted:
                for k in feeds:
                    if chunks[k][1] == e:
                        pass_on(k, z - (positions - 1) * out, [to_side])
                sides_of(e)
                own_hidden(e)
        for k in downs:
            pass_on(k, z - (positions - 1) * out, [to_side])
        for k in range(len(chunks)):
            if k not in everywhere:
                copy_own(k).wait()

    @pl.when(jnp.logical_not(end))
    def _():
        def beyond(k):
            return [to_out] if k in everywhere else []

        for k in range(len(chunks)):
            send(k, dp, source(k), *to_in).start()
        for k in everywhere:
            send(k, dp, source(k), *to_out).start()
        for k in range(len(chunks)):
            send(k, dp, source(k), *to_side).start()

        def from_outer(k):
            pass_on(k, z + out, [to_in, to_side])

        def from_near(k):
            pass_on(k, z - out, beyond(k) + [to_side])

        def from_far(k):
            pass_on(k, z - 2 * out, beyond(k) + [to_side])

        load_x.wait()
        norm(x, x, 0, rows, 8)
        for p in range(PIECES):
            token_arrived(tp, p)
            token_copy(guest, tp, p, 0, (dp, along_x)).start()
            token_copy(guest, tp, p, 1, (dp, along_y)).start()
            from_near(p)
        norm_quarter(tp)
        for p in range(PIECES):
            token_arrived(along_x, p)
            if p < PIECES // 2:
                token_copy(guest, along_x, p, 2, (dp, along_y)).start()
            token_arrived(along_y, p)
            if p >= PIECES // 2:
                token_copy(guest, along_y, p, 2, (dp, along_x)).start()
            if p == 1:
                score()
                for k in downs:
                    from_near(k)
            if p == 2:
                from_outer(feeds[0])
        from_outer(feeds[1])
        norm_quarter(along_x)
        norm_quarter(along_y)
        from_far(feeds[0])
        from_outer(feeds[2])
        for p in range(PIECES):
            token_arrived(across, p)
        norm_quarter(across)
        from_far(feeds[1])
        from_outer(feeds[3])
        sides_of(order[0])
        guest_hidden(order[0])
        from_outer(downs[0])
        from_far(feeds[2])
        own_hidden(order[0])
        from_outer(downs[1])
        from_far(feeds[3])
        sides_of(order[1])
        if order[1] in hosted:
            guest_hidden(order[1])
        own_hidden(order[1])
        for k in downs:
            from_far(k)

    for k in downs:
        wait_side(k)
    for e in order:
        for i in range(1, tps):
            s = lax.rem(tp + i, tps)
            pltpu.make_async_remote_copy(
                src_ref=hid.at[e, s], dst_ref=hid.at[e, s], send_sem=hid_send.at[e, i - 1],
                recv_sem=hid_recv.at[e, s], device_id=side, device_id_type=MESH,
            ).wait_recv()
    down()

    def sent(k, p, sem):
        d = p * CORES + core
        send(k, d, slot(k, d), sem, side).wait_send()

    for e in range(experts):
        for i in range(1, tps):
            send_hidden(e, i).wait_send()
    for k in range(len(chunks)):
        sent(k, z, in_sem)

    @pl.when(end)
    def _():
        for p in range(PIECES):
            token_copy(x_hbm, tp, p, 0, inner).wait_send()
        for k in everywhere:
            for p in range(positions):
                sent(k, p, side_sem)

    @pl.when(jnp.logical_not(end))
    def _():
        for p in range(PIECES):
            for kind in range(3):
                token_copy(guest, tp, p, kind, side).wait_send()
        for e in hosted:
            send_back(e).wait_send()
        for k in range(len(chunks)):
            sent(k, z + out, in_sem)
            for p in range(positions):
                sent(k, p, side_sem)
        for k in everywhere:
            sent(k, z, out_sem)
            sent(k, z - out, out_sem)
            sent(k, z - 2 * out, out_sem)


def streamed(groups, tps, tokens, gain, router, routes, w_gate, w_up, w_down):
    rows, depth = tokens.shape
    experts, shard, width = w_gate.shape
    down_rows, cols = w_down.shape[1:]
    positions = groups // CORES
    vmem = pl.BlockSpec(memory_space=pltpu.VMEM)
    hbm = pl.BlockSpec(memory_space=pl.ANY)
    chunks = 3 * experts
    dma = pltpu.SemaphoreType.DMA
    return pl.pallas_call(
        functools.partial(kernel, groups, tps, HOSTED),
        out_shape=jax.ShapeDtypeStruct((rows, cols), jnp.bfloat16),
        in_specs=[hbm, vmem, vmem, vmem, hbm, hbm, hbm],
        out_specs=vmem,
        scratch_shapes=[
            pltpu.VMEM((rows, depth), jnp.bfloat16),
            pltpu.VMEM((rows, depth), jnp.bfloat16),
            pltpu.VMEM((rows, depth), jnp.bfloat16),
            pltpu.VMEM((2, experts, groups, shard, width), jnp.bfloat16),
            pltpu.VMEM((experts, groups, down_rows, cols), jnp.bfloat16),
            pltpu.VMEM((experts, tps, rows, width), jnp.bfloat16),
            pltpu.VMEM((experts, rows, width), jnp.bfloat16),
            pltpu.VMEM((rows, router.shape[1]), jnp.float32),
            dma,
            dma((chunks,)),
            dma((chunks, groups)),
            dma((chunks, positions)),
            dma((chunks, positions)),
            dma((chunks, positions)),
            dma((experts, tps - 1)),
            dma((experts, tps)),
            dma((3, PIECES)),
            dma((tps, PIECES)),
            dma((experts,)),
            dma((experts,)),
        ],
        compiler_params=pltpu.CompilerParams(
            collective_id=0, has_side_effects=True, vmem_limit_bytes=60 * 1024 * 1024
        ),
    )(tokens, gain.reshape(1, -1), router.T, routes.T, w_gate, w_up, w_down)


def solution(mesh):
    groups, tps = mesh.shape["dp"], mesh.shape["tp"]
    fits = groups == 4 * CORES and tps == 4
    body = functools.partial(streamed, groups, tps) if fits else gathered
    return jax.shard_map(
        body,
        mesh=mesh,
        in_specs=(
            P("dp", None),
            P(),
            P(),
            P("dp", None),
            P(None, "dp", "tp"),
            P(None, "dp", "tp"),
            P(None, "dp", "tp"),
        ),
        out_specs=P("dp", "tp"),
        check_vma=False,
    )
```

```python
import functools

import jax
import jax.numpy as jnp
from jax import lax
from jax.experimental import pallas as pl
from jax.experimental.pallas import tpu as pltpu
from jax.sharding import PartitionSpec as P

EPS = 1e-06
ROUTE_SCALE = 2.5
MESH = pl.DeviceIdType.MESH
CORES = 2
PIECES = 4
HALVES = 2
HOSTED = (0, 1)


def gathered(tokens, gain, router, routes, w_gate, w_up, w_down):
    values = tokens.astype(jnp.float32)
    square = jnp.mean(values * values, axis=-1, keepdims=True)
    normed = (values * lax.rsqrt(square + EPS) * gain).astype(jnp.bfloat16)
    scores = jax.nn.sigmoid(
        jnp.dot(normed.astype(jnp.float32), router, precision=lax.Precision.HIGHEST)
    )
    labels = jnp.arange(router.shape[1], dtype=jnp.int32)
    picked_mask = (routes[:, :, None] == labels[None, None, :]).astype(jnp.float32)
    picked = jnp.sum(picked_mask * scores[:, None, :], axis=-1)
    chosen = jnp.sum(picked_mask, axis=1)
    combine = chosen * scores * ROUTE_SCALE / jnp.sum(picked, axis=-1, keepdims=True)
    held_weights = combine[:, : w_gate.shape[0]]
    full_gate, full_up, full_down = (
        lax.all_gather(w_gate, "dp", axis=1, tiled=True),
        lax.all_gather(w_up, "dp", axis=1, tiled=True),
        lax.all_gather(w_down, "dp", axis=1, tiled=True),
    )
    gate_value = jnp.einsum("td,edf->tef", normed, full_gate, preferred_element_type=jnp.float32)
    up_value = jnp.einsum("td,edf->tef", normed, full_up, preferred_element_type=jnp.float32)
    hidden = (jax.nn.silu(gate_value) * up_value * held_weights[:, :, None]).astype(jnp.bfloat16)
    whole_hidden = lax.all_gather(hidden, "tp", axis=2, tiled=True)
    mixed = jnp.einsum("tef,efd->td", whole_hidden, full_down, preferred_element_type=jnp.float32)
    return mixed.astype(jnp.bfloat16)


def kernel(
    groups, tps, hosted, x_hbm, gain_ref, router_ref, routes_ref, wg_hbm, wu_hbm, wd_hbm, o_ref,
    x, guest, guest_normed, w, dn, hid, guest_hid, comb, total,
    x_sem, own_sem, recv_sem, in_sem, out_sem, side_sem, hid_send, hid_recv,
    tok_send, tok_recv, back_send, back_recv,
):
    dp, tp = lax.axis_index("dp"), lax.axis_index("tp")
    positions = groups // CORES
    z, core = dp // CORES, dp % CORES
    experts = wg_hbm.shape[0]
    rows = x.shape[0]
    end = jnp.logical_or(z == positions - 1, z == 0)
    out = 2 * (2 * z // positions) - 1

    def at(p):
        return (p * CORES + core, tp)

    inner = at(z - out)
    outer = at(jnp.clip(z + out, 0, positions - 1))
    side = (z * CORES + (1 - core), tp)
    along_x = tp + 1 - 2 * (tp % 2)
    along_y = lax.rem(tp + 2, tps)
    across = lax.rem(along_x + 2, tps)

    load_x = pltpu.make_async_copy(x_hbm, x, x_sem)
    load_x.start()
    order = sorted(range(experts), key=lambda e: e not in hosted)
    chunks = [(m, e, 0) for e in order for m in (0, 1)]
    feeds = list(range(len(chunks)))
    chunks += [(2, e, h) for e in order for h in range(HALVES)]
    downs = [k for k in range(len(chunks)) if k not in feeds]
    everywhere = [k for k, (m, e, _) in enumerate(chunks) if m == 2 or e not in hosted]
    half = dn.shape[2] // HALVES
    strip = rows // HALVES

    def source(k):
        m, e, h = chunks[k]
        return wd_hbm.at[e, pl.ds(h * half, half)] if m == 2 else (wg_hbm, wu_hbm)[m].at[e]

    def slot(k, d):
        m, e, h = chunks[k]
        return dn.at[e, d, pl.ds(h * half, half)] if m == 2 else w.at[m, e, d]

    def copy_own(k):
        return pltpu.make_async_copy(source(k), slot(k, dp), own_sem.at[k])

    for k in range(len(chunks)):
        copy_own(k).start()

    barrier = pltpu.get_barrier_semaphore()
    pl.semaphore_signal(barrier, inc=1, device_id=side, device_id_type=MESH)
    pl.semaphore_signal(barrier, inc=1, device_id=inner, device_id_type=MESH)
    for i in range(1, tps):
        pl.semaphore_signal(
            barrier, inc=1, device_id=(dp, lax.rem(tp + i, tps)), device_id_type=MESH
        )

    @pl.when(jnp.logical_not(end))
    def _():
        pl.semaphore_signal(barrier, inc=1, device_id=outer, device_id_type=MESH)

    pl.semaphore_wait(barrier, tps + 2 - jnp.where(end, 1, 0))

    def send(k, d, src, sem, to):
        return pltpu.make_async_remote_copy(
            src_ref=src, dst_ref=slot(k, d), send_sem=sem.at[k, d // CORES],
            recv_sem=recv_sem.at[k, d], device_id=to, device_id_type=MESH,
        )

    def arrived(k, d):
        send(k, d, slot(k, d), side_sem, side).wait_recv()

    def pass_on(k, p, targets):
        d = p * CORES + core
        arrived(k, d)
        for sem, to in targets:
            send(k, d, slot(k, d), sem, to).start()

    def wait_side(k):
        for p in range(positions):
            arrived(k, p * CORES + (1 - core))
        copy_own(k).wait()

    quarter = rows // tps
    piece = quarter // PIECES

    def token_part(q, p):
        return pl.ds(pl.multiple_of(q * quarter + p * piece, piece), piece)

    def token_copy(src, q, p, kind, to):
        return pltpu.make_async_remote_copy(
            src_ref=src.at[token_part(q, p)], dst_ref=guest.at[token_part(q, p)],
            send_sem=tok_send.at[kind, p], recv_sem=tok_recv.at[q, p],
            device_id=to, device_id_type=MESH,
        )

    def token_arrived(q, p):
        token_copy(guest, q, p, 0, side).wait_recv()

    def norm(src, dst, start, count, steps):
        step = count // steps

        def body(i, _):
            part = pl.ds(pl.multiple_of(start + i * step, step), step)
            v = src[part, :].astype(jnp.float32)
            square = jnp.mean(v * v, axis=-1, keepdims=True)
            dst[part, :] = (v * lax.rsqrt(square + EPS) * gain_ref[...]).astype(jnp.bfloat16)
            return 0

        lax.fori_loop(0, steps, body, 0)

    def norm_quarter(q):
        norm(guest, guest_normed, q * quarter, quarter, 2)

    def score():
        rest = router_ref[...]
        logits = jnp.zeros((rows, rest.shape[0]), jnp.float32)
        parts = []
        for _ in range(3):
            part = rest.astype(jnp.bfloat16)
            rest = rest - part.astype(jnp.float32)
            parts.append(part)
        for part in parts[::-1]:
            logits += lax.dot_general(
                x[...], part, (((1,), (1,)), ((), ())), preferred_element_type=jnp.float32
            )
        scores = 1.0 / (1.0 + jnp.exp(-logits))
        routed = scores.shape[1]
        picks = routes_ref[...].astype(jnp.float32)
        labels = lax.broadcasted_iota(jnp.int32, scores.shape, 1).astype(jnp.float32)
        chosen = jnp.zeros_like(scores)
        for i in range(routes_ref.shape[0]):
            column = jnp.transpose(jnp.broadcast_to(picks[i : i + 1, :], (128, rows)))
            chosen += jnp.where(column[:, :routed] == labels, 1.0, 0.0)
        picked = chosen * scores
        comb[...] = picked * ROUTE_SCALE / jnp.sum(picked, axis=-1, keepdims=True)

    def send_hidden(e, h, i):
        part = pl.ds(h * strip, strip)
        return pltpu.make_async_remote_copy(
            src_ref=hid.at[e, tp, part], dst_ref=hid.at[e, tp, part],
            send_sem=hid_send.at[e, h, i - 1], recv_sem=hid_recv.at[e, h, tp],
            device_id=(dp, lax.rem(tp + i, tps)), device_id_type=MESH,
        )

    def share_hidden(e, h):
        for i in range(1, tps):
            send_hidden(e, h, i).start()

    def wait_hidden(e):
        for h in range(HALVES):
            part = pl.ds(h * strip, strip)
            for i in range(1, tps):
                s = lax.rem(tp + i, tps)
                pltpu.make_async_remote_copy(
                    src_ref=hid.at[e, s, part], dst_ref=hid.at[e, s, part],
                    send_sem=hid_send.at[e, h, i - 1], recv_sem=hid_recv.at[e, h, s],
                    device_id=side, device_id_type=MESH,
                ).wait_recv()

    def send_back(e, h):
        part = pl.ds(h * strip, strip)
        return pltpu.make_async_remote_copy(
            src_ref=guest_hid.at[e, part], dst_ref=hid.at[e, tp, part],
            send_sem=back_send.at[e, h], recv_sem=back_recv.at[e, h],
            device_id=outer, device_id_type=MESH,
        )

    def expert_hidden(e, h, src, dst):
        part = pl.ds(h * strip, strip)
        lhs = src[part, :]
        depth = x.shape[1]
        gate = jnp.dot(
            lhs, w[0, e].reshape(depth, w.shape[-1]), preferred_element_type=jnp.float32
        )
        up = jnp.dot(
            lhs, w[1, e].reshape(depth, w.shape[-1]), preferred_element_type=jnp.float32
        )
        dst[part, :] = (gate / (1.0 + jnp.exp(-gate)) * up).astype(jnp.bfloat16)

    def own_hidden(e):
        for h in range(HALVES):
            expert_hidden(e, h, x, hid.at[e, tp])
            share_hidden(e, h)

    def guest_hidden(e):
        for h in range(HALVES):
            expert_hidden(e, h, guest_normed, guest_hid.at[e])
            send_back(e, h).start()

    def sides_of(e):
        for k in feeds:
            if chunks[k][1] == e:
                wait_side(k)

    def down(e):
        cols = o_ref.shape[1]
        step = cols // 4
        wait_hidden(e)
        for k in downs:
            if chunks[k][1] == e:
                wait_side(k)

        def body(i, _):
            part = pl.ds(pl.multiple_of(i * step, step), step)
            lhs = jnp.concatenate([hid[e, t] for t in range(tps)], axis=1)
            rhs = dn[e, :, :, part].reshape(lhs.shape[1], step)
            term = jnp.dot(lhs, rhs, preferred_element_type=jnp.float32)
            term = term * comb[:, e : e + 1]
            if e != order[0]:
                term += total[:, part]
            if e == order[-1]:
                o_ref[:, part] = term.astype(o_ref.dtype)
            else:
                total[:, part] = term
            return 0

        lax.fori_loop(0, 4, body, 0)

    to_in, to_out, to_side = (in_sem, inner), (out_sem, outer), (side_sem, side)

    @pl.when(end)
    def _():
        for p in range(PIECES):
            token_copy(x_hbm, tp, p, 0, inner).start()
        for k in range(len(chunks)):
            send(k, dp, source(k), *to_in).start()
        for k in everywhere:
            send(k, dp, source(k), *to_side).start()
        load_x.wait()
        norm(x, x, 0, rows, 8)
        score()
        for k in everywhere:
            pass_on(k, z - out, [to_side])
        for k in everywhere[:-1]:
            pass_on(k, z - 2 * out, [to_side])
        for e in order:
            if e in hosted:
                for h in range(HALVES):
                    send_back(e, h).wait_recv()
                    share_hidden(e, h)
        pass_on(everywhere[-1], z - 2 * out, [to_side])
        for e in order:
            if e not in hosted:
                for k in feeds:
                    if chunks[k][1] == e:
                        pass_on(k, z - 3 * out, [to_side])
                sides_of(e)
                own_hidden(e)
        for e in order:
            for k in downs:
                if chunks[k][1] == e:
                    pass_on(k, z - 3 * out, [to_side])
            down(e)
        for k in range(len(chunks)):
            if k not in everywhere:
                copy_own(k).wait()

    @pl.when(jnp.logical_not(end))
    def _():
        def beyond(k):
            return [to_out] if k in everywhere else []

        for k in range(len(chunks) - 1):
            send(k, dp, source(k), *to_in).start()
        for k in everywhere:
            send(k, dp, source(k), *to_out).start()
        for k in range(len(chunks)):
            send(k, dp, source(k), *to_side).start()

        def from_outer(k):
            pass_on(k, z + out, [to_in, to_side])

        def from_near(k):
            pass_on(k, z - out, beyond(k) + [to_side])

        def from_far(k):
            pass_on(k, z - 2 * out, beyond(k) + [to_side])

        load_x.wait()
        norm(x, x, 0, rows, 8)
        for p in range(PIECES):
            token_arrived(tp, p)
            token_copy(guest, tp, p, 0, (dp, along_x)).start()
            token_copy(guest, tp, p, 1, (dp, along_y)).start()
            from_near(p)
        norm_quarter(tp)
        for p in range(PIECES):
            token_arrived(along_x, p)
            if p < PIECES // 2:
                token_copy(guest, along_x, p, 2, (dp, along_y)).start()
            token_arrived(along_y, p)
            if p >= PIECES // 2:
                token_copy(guest, along_y, p, 2, (dp, along_x)).start()
            if p == 0:
                from_near(downs[0])
                from_near(downs[1])
            if p == 1:
                score()
                from_near(downs[2])
            if p == 2:
                from_outer(feeds[0])
        from_outer(feeds[1])
        norm_quarter(along_x)
        norm_quarter(along_y)
        from_far(feeds[0])
        from_outer(feeds[2])
        from_far(feeds[1])
        for p in range(PIECES):
            token_arrived(across, p)
        norm_quarter(across)
        from_outer(feeds[3])
        send(len(chunks) - 1, dp, source(len(chunks) - 1), *to_in).start()
        sides_of(order[0])
        guest_hidden(order[0])
        from_far(feeds[2])
        from_outer(downs[0])
        own_hidden(order[0])
        from_outer(downs[1])
        from_far(feeds[3])
        sides_of(order[1])
        if order[1] in hosted:
            guest_hidden(order[1])
        from_outer(downs[2])
        from_near(downs[3])
        own_hidden(order[1])
        from_outer(downs[3])
        for e in order:
            for k in downs:
                if chunks[k][1] == e:
                    from_far(k)
            down(e)

    def sent(k, p, sem):
        d = p * CORES + core
        send(k, d, slot(k, d), sem, side).wait_send()

    for e in range(experts):
        for h in range(HALVES):
            for i in range(1, tps):
                send_hidden(e, h, i).wait_send()
    for k in range(len(chunks)):
        sent(k, z, in_sem)

    @pl.when(end)
    def _():
        for p in range(PIECES):
            token_copy(x_hbm, tp, p, 0, inner).wait_send()
        for k in everywhere:
            for p in range(positions):
                sent(k, p, side_sem)

    @pl.when(jnp.logical_not(end))
    def _():
        for p in range(PIECES):
            for kind in range(3):
                token_copy(guest, tp, p, kind, side).wait_send()
        for e in hosted:
            for h in range(HALVES):
                send_back(e, h).wait_send()
        for k in range(len(chunks)):
            sent(k, z + out, in_sem)
            for p in range(positions):
                sent(k, p, side_sem)
        for k in everywhere:
            sent(k, z, out_sem)
            sent(k, z - out, out_sem)
            sent(k, z - 2 * out, out_sem)


def streamed(groups, tps, tokens, gain, router, routes, w_gate, w_up, w_down):
    rows, depth = tokens.shape
    experts, shard, width = w_gate.shape
    down_rows, cols = w_down.shape[1:]
    positions = groups // CORES
    vmem = pl.BlockSpec(memory_space=pltpu.VMEM)
    hbm = pl.BlockSpec(memory_space=pl.ANY)
    chunks = (2 + HALVES) * experts
    dma = pltpu.SemaphoreType.DMA
    return pl.pallas_call(
        functools.partial(kernel, groups, tps, HOSTED),
        out_shape=jax.ShapeDtypeStruct((rows, cols), jnp.bfloat16),
        in_specs=[hbm, vmem, vmem, vmem, hbm, hbm, hbm],
        out_specs=vmem,
        scratch_shapes=[
            pltpu.VMEM((rows, depth), jnp.bfloat16),
            pltpu.VMEM((rows, depth), jnp.bfloat16),
            pltpu.VMEM((rows, depth), jnp.bfloat16),
            pltpu.VMEM((2, experts, groups, shard, width), jnp.bfloat16),
            pltpu.VMEM((experts, groups, down_rows, cols), jnp.bfloat16),
            pltpu.VMEM((experts, tps, rows, width), jnp.bfloat16),
            pltpu.VMEM((experts, rows, width), jnp.bfloat16),
            pltpu.VMEM((rows, router.shape[1]), jnp.float32),
            pltpu.VMEM((rows, cols), jnp.float32),
            dma,
            dma((chunks,)),
            dma((chunks, groups)),
            dma((chunks, positions)),
            dma((chunks, positions)),
            dma((chunks, positions)),
            dma((experts, HALVES, tps - 1)),
            dma((experts, HALVES, tps)),
            dma((3, PIECES)),
            dma((tps, PIECES)),
            dma((experts, HALVES)),
            dma((experts, HALVES)),
        ],
        compiler_params=pltpu.CompilerParams(
            collective_id=0, has_side_effects=True, vmem_limit_bytes=60 * 1024 * 1024
        ),
    )(tokens, gain.reshape(1, -1), router.T, routes.T, w_gate, w_up, w_down)


def solution(mesh):
    groups, tps = mesh.shape["dp"], mesh.shape["tp"]
    fits = groups == 4 * CORES and tps == 4
    body = functools.partial(streamed, groups, tps) if fits else gathered
    return jax.shard_map(
        body,
        mesh=mesh,
        in_specs=(
            P("dp", None),
            P(),
            P(),
            P("dp", None),
            P(None, "dp", "tp"),
            P(None, "dp", "tp"),
            P(None, "dp", "tp"),
        ),
        out_specs=P("dp", "tp"),
        check_vma=False,
    )
```

```python
import functools

import jax
import jax.numpy as jnp
from jax import lax
from jax.experimental import pallas as pl
from jax.experimental.pallas import tpu as pltpu
from jax.sharding import PartitionSpec as P

EPS = 1e-06
ROUTE_SCALE = 2.5
MESH = pl.DeviceIdType.MESH
CORES = 2
PIECES = 4
HALVES = 2
HOSTED = (0, 1)


def gathered(tokens, gain, router, routes, w_gate, w_up, w_down):
    values = tokens.astype(jnp.float32)
    square = jnp.mean(values * values, axis=-1, keepdims=True)
    normed = (values * lax.rsqrt(square + EPS) * gain).astype(jnp.bfloat16)
    scores = jax.nn.sigmoid(
        jnp.dot(normed.astype(jnp.float32), router, precision=lax.Precision.HIGHEST)
    )
    labels = jnp.arange(router.shape[1], dtype=jnp.int32)
    picked_mask = (routes[:, :, None] == labels[None, None, :]).astype(jnp.float32)
    picked = jnp.sum(picked_mask * scores[:, None, :], axis=-1)
    chosen = jnp.sum(picked_mask, axis=1)
    combine = chosen * scores * ROUTE_SCALE / jnp.sum(picked, axis=-1, keepdims=True)
    held_weights = combine[:, : w_gate.shape[0]]
    full_gate, full_up, full_down = (
        lax.all_gather(w_gate, "dp", axis=1, tiled=True),
        lax.all_gather(w_up, "dp", axis=1, tiled=True),
        lax.all_gather(w_down, "dp", axis=1, tiled=True),
    )
    gate_value = jnp.einsum("td,edf->tef", normed, full_gate, preferred_element_type=jnp.float32)
    up_value = jnp.einsum("td,edf->tef", normed, full_up, preferred_element_type=jnp.float32)
    hidden = (jax.nn.silu(gate_value) * up_value * held_weights[:, :, None]).astype(jnp.bfloat16)
    whole_hidden = lax.all_gather(hidden, "tp", axis=2, tiled=True)
    mixed = jnp.einsum("tef,efd->td", whole_hidden, full_down, preferred_element_type=jnp.float32)
    return mixed.astype(jnp.bfloat16)


def kernel(
    groups, tps, hosted, x_hbm, gain_ref, router_ref, routes_ref, wg_hbm, wu_hbm, wd_hbm, o_ref,
    x, guest, guest_normed, w, dn, hid, guest_hid, comb, total,
    x_sem, own_sem, recv_sem, in_sem, out_sem, side_sem, hid_send, hid_recv,
    tok_send, tok_recv, back_send, back_recv,
):
    dp, tp = lax.axis_index("dp"), lax.axis_index("tp")
    positions = groups // CORES
    z, core = dp // CORES, dp % CORES
    experts = wg_hbm.shape[0]
    rows = x.shape[0]
    end = jnp.logical_or(z == positions - 1, z == 0)
    out = 2 * (2 * z // positions) - 1

    def at(p):
        return (p * CORES + core, tp)

    inner = at(z - out)
    outer = at(jnp.clip(z + out, 0, positions - 1))
    side = (z * CORES + (1 - core), tp)
    along_x = tp + 1 - 2 * (tp % 2)
    along_y = lax.rem(tp + 2, tps)
    across = lax.rem(along_x + 2, tps)

    load_x = pltpu.make_async_copy(x_hbm, x, x_sem)
    load_x.start()
    order = sorted(range(experts), key=lambda e: e not in hosted)
    chunks = [(m, e, 0) for e in order for m in (0, 1)]
    feeds = list(range(len(chunks)))
    chunks += [(2, e, h) for e in order for h in range(HALVES)]
    downs = [k for k in range(len(chunks)) if k not in feeds]
    everywhere = [k for k, (m, e, _) in enumerate(chunks) if m == 2 or e not in hosted]
    half = dn.shape[2] // HALVES
    strip = rows // HALVES

    def source(k):
        m, e, h = chunks[k]
        return wd_hbm.at[e, pl.ds(h * half, half)] if m == 2 else (wg_hbm, wu_hbm)[m].at[e]

    def slot(k, d):
        m, e, h = chunks[k]
        return dn.at[e, d, pl.ds(h * half, half)] if m == 2 else w.at[m, e, d]

    def copy_own(k):
        return pltpu.make_async_copy(source(k), slot(k, dp), own_sem.at[k])

    for k in range(len(chunks)):
        copy_own(k).start()

    barrier = pltpu.get_barrier_semaphore()
    pl.semaphore_signal(barrier, inc=1, device_id=side, device_id_type=MESH)
    pl.semaphore_signal(barrier, inc=1, device_id=inner, device_id_type=MESH)
    for i in range(1, tps):
        pl.semaphore_signal(
            barrier, inc=1, device_id=(dp, lax.rem(tp + i, tps)), device_id_type=MESH
        )

    @pl.when(jnp.logical_not(end))
    def _():
        pl.semaphore_signal(barrier, inc=1, device_id=outer, device_id_type=MESH)

    pl.semaphore_wait(barrier, tps + 2 - jnp.where(end, 1, 0))

    def send(k, d, src, sem, to):
        return pltpu.make_async_remote_copy(
            src_ref=src, dst_ref=slot(k, d), send_sem=sem.at[k, d // CORES],
            recv_sem=recv_sem.at[k, d], device_id=to, device_id_type=MESH,
        )

    def arrived(k, d):
        send(k, d, slot(k, d), side_sem, side).wait_recv()

    def pass_on(k, p, targets):
        d = p * CORES + core
        arrived(k, d)
        for sem, to in targets:
            send(k, d, slot(k, d), sem, to).start()

    def wait_side(k):
        for p in range(positions):
            arrived(k, p * CORES + (1 - core))
        copy_own(k).wait()

    quarter = rows // tps
    piece = quarter // PIECES

    def token_part(q, p):
        return pl.ds(pl.multiple_of(q * quarter + p * piece, piece), piece)

    def token_copy(src, q, p, kind, to):
        return pltpu.make_async_remote_copy(
            src_ref=src.at[token_part(q, p)], dst_ref=guest.at[token_part(q, p)],
            send_sem=tok_send.at[kind, p], recv_sem=tok_recv.at[q, p],
            device_id=to, device_id_type=MESH,
        )

    def token_arrived(q, p):
        token_copy(guest, q, p, 0, side).wait_recv()

    def norm(src, dst, start, count, steps):
        step = count // steps

        def body(i, _):
            part = pl.ds(pl.multiple_of(start + i * step, step), step)
            v = src[part, :].astype(jnp.float32)
            square = jnp.mean(v * v, axis=-1, keepdims=True)
            dst[part, :] = (v * lax.rsqrt(square + EPS) * gain_ref[...]).astype(jnp.bfloat16)
            return 0

        lax.fori_loop(0, steps, body, 0)

    def norm_quarter(q):
        norm(guest, guest_normed, q * quarter, quarter, 2)

    def score():
        rest = router_ref[...]
        logits = jnp.zeros((rows, rest.shape[0]), jnp.float32)
        parts = []
        for _ in range(3):
            part = rest.astype(jnp.bfloat16)
            rest = rest - part.astype(jnp.float32)
            parts.append(part)
        for part in parts[::-1]:
            logits += lax.dot_general(
                x[...], part, (((1,), (1,)), ((), ())), preferred_element_type=jnp.float32
            )
        scores = 1.0 / (1.0 + jnp.exp(-logits))
        routed = scores.shape[1]
        picks = routes_ref[...].astype(jnp.float32)
        labels = lax.broadcasted_iota(jnp.int32, scores.shape, 1).astype(jnp.float32)
        chosen = jnp.zeros_like(scores)
        for i in range(routes_ref.shape[0]):
            column = jnp.transpose(jnp.broadcast_to(picks[i : i + 1, :], (128, rows)))
            chosen += jnp.where(column[:, :routed] == labels, 1.0, 0.0)
        picked = chosen * scores
        comb[...] = picked * ROUTE_SCALE / jnp.sum(picked, axis=-1, keepdims=True)

    def hidden_copy(e, h, t, kind, to):
        part = pl.ds(h * strip, strip)
        return pltpu.make_async_remote_copy(
            src_ref=hid.at[e, t, part], dst_ref=hid.at[e, t, part],
            send_sem=hid_send.at[e, h, kind], recv_sem=hid_recv.at[e, h, t],
            device_id=(dp, to), device_id_type=MESH,
        )

    def share_hidden(e, h):
        hidden_copy(e, h, tp, 0, along_x).start()
        hidden_copy(e, h, tp, 1, along_y).start()

    def relay_hidden(e):
        for h, (t, to) in enumerate(((along_x, along_y), (along_y, along_x))):
            hidden_copy(e, h, t, 2, to).wait_recv()
            hidden_copy(e, h, t, 2, to).start()

    def wait_hidden(e):
        for h, t in ((0, along_y), (1, along_x), (0, across), (1, across)):
            hidden_copy(e, h, t, 2, along_x).wait_recv()

    def send_back(e, h):
        part = pl.ds(h * strip, strip)
        return pltpu.make_async_remote_copy(
            src_ref=guest_hid.at[e, part], dst_ref=hid.at[e, tp, part],
            send_sem=back_send.at[e, h], recv_sem=back_recv.at[e, h],
            device_id=outer, device_id_type=MESH,
        )

    def expert_hidden(e, h, src, dst):
        part = pl.ds(h * strip, strip)
        lhs = src[part, :]
        depth = x.shape[1]
        gate = jnp.dot(
            lhs, w[0, e].reshape(depth, w.shape[-1]), preferred_element_type=jnp.float32
        )
        up = jnp.dot(
            lhs, w[1, e].reshape(depth, w.shape[-1]), preferred_element_type=jnp.float32
        )
        dst[part, :] = (gate / (1.0 + jnp.exp(-gate)) * up).astype(jnp.bfloat16)

    def own_hidden(e):
        for h in range(HALVES):
            expert_hidden(e, h, x, hid.at[e, tp])
            share_hidden(e, h)

    def guest_hidden(e):
        for h in range(HALVES):
            expert_hidden(e, h, guest_normed, guest_hid.at[e])
            send_back(e, h).start()

    def sides_of(e):
        for k in feeds:
            if chunks[k][1] == e:
                wait_side(k)

    def down(e):
        cols = o_ref.shape[1]
        step = cols // 4
        wait_hidden(e)
        for k in downs:
            if chunks[k][1] == e:
                wait_side(k)

        def body(i, _):
            part = pl.ds(pl.multiple_of(i * step, step), step)
            lhs = jnp.concatenate([hid[e, t] for t in range(tps)], axis=1)
            rhs = dn[e, :, :, part].reshape(lhs.shape[1], step)
            term = jnp.dot(lhs, rhs, preferred_element_type=jnp.float32)
            term = term * comb[:, e : e + 1]
            if e != order[0]:
                term += total[:, part]
            if e == order[-1]:
                o_ref[:, part] = term.astype(o_ref.dtype)
            else:
                total[:, part] = term
            return 0

        lax.fori_loop(0, 4, body, 0)

    to_in, to_out, to_side = (in_sem, inner), (out_sem, outer), (side_sem, side)

    @pl.when(end)
    def _():
        for p in range(PIECES):
            token_copy(x_hbm, tp, p, 0, inner).start()
        for k in range(len(chunks)):
            send(k, dp, source(k), *to_in).start()
        for k in everywhere:
            send(k, dp, source(k), *to_side).start()
        load_x.wait()
        norm(x, x, 0, rows, 8)
        score()
        for k in everywhere:
            pass_on(k, z - out, [to_side])
        for k in everywhere[:-1]:
            pass_on(k, z - 2 * out, [to_side])
        for e in order:
            if e in hosted:
                for h in range(HALVES):
                    send_back(e, h).wait_recv()
                    share_hidden(e, h)
                relay_hidden(e)
        pass_on(everywhere[-1], z - 2 * out, [to_side])
        for e in order:
            if e not in hosted:
                for k in feeds:
                    if chunks[k][1] == e:
                        pass_on(k, z - 3 * out, [to_side])
                sides_of(e)
                own_hidden(e)
                relay_hidden(e)
        for e in order:
            for k in downs:
                if chunks[k][1] == e:
                    pass_on(k, z - 3 * out, [to_side])
            down(e)
        for k in range(len(chunks)):
            if k not in everywhere:
                copy_own(k).wait()

    @pl.when(jnp.logical_not(end))
    def _():
        def beyond(k):
            return [to_out] if k in everywhere else []

        for k in range(len(chunks) - 1):
            send(k, dp, source(k), *to_in).start()
        for k in everywhere:
            send(k, dp, source(k), *to_out).start()
        for k in range(len(chunks)):
            send(k, dp, source(k), *to_side).start()

        def from_outer(k):
            pass_on(k, z + out, [to_in, to_side])

        def from_near(k):
            pass_on(k, z - out, beyond(k) + [to_side])

        def from_far(k):
            pass_on(k, z - 2 * out, beyond(k) + [to_side])

        load_x.wait()
        norm(x, x, 0, rows, 8)
        score()
        for p in range(PIECES):
            token_arrived(tp, p)
            token_copy(guest, tp, p, 0, (dp, along_x)).start()
            token_copy(guest, tp, p, 1, (dp, along_y)).start()
            from_near(p)
        norm_quarter(tp)
        for p in range(PIECES):
            token_arrived(along_x, p)
            if p < PIECES // 2:
                token_copy(guest, along_x, p, 2, (dp, along_y)).start()
            token_arrived(along_y, p)
            if p >= PIECES // 2:
                token_copy(guest, along_y, p, 2, (dp, along_x)).start()
            if p == 0:
                from_near(downs[0])
                from_near(downs[1])
            if p == 1:
                from_near(downs[2])
            if p == 2:
                from_outer(feeds[0])
        norm_quarter(along_x)
        from_outer(feeds[1])
        norm_quarter(along_y)
        from_far(feeds[0])
        from_outer(feeds[2])
        for p in range(PIECES):
            token_arrived(across, p)
        norm_quarter(across)
        from_far(feeds[1])
        sides_of(order[0])
        own_hidden(order[0])
        from_outer(feeds[3])
        send(len(chunks) - 1, dp, source(len(chunks) - 1), *to_in).start()
        guest_hidden(order[0])
        from_far(feeds[2])
        from_outer(downs[0])
        from_outer(downs[1])
        relay_hidden(order[0])
        from_far(feeds[3])
        sides_of(order[1])
        if order[1] in hosted:
            guest_hidden(order[1])
        from_outer(downs[2])
        from_near(downs[3])
        own_hidden(order[1])
        from_outer(downs[3])
        from_far(downs[0])
        relay_hidden(order[1])
        for k in downs[1:]:
            from_far(k)
        for e in order:
            down(e)

    def sent(k, p, sem):
        d = p * CORES + core
        send(k, d, slot(k, d), sem, side).wait_send()

    for e in range(experts):
        for h in range(HALVES):
            for kind in range(3):
                hidden_copy(e, h, tp, kind, along_x).wait_send()
    for k in range(len(chunks)):
        sent(k, z, in_sem)

    @pl.when(end)
    def _():
        for p in range(PIECES):
            token_copy(x_hbm, tp, p, 0, inner).wait_send()
        for k in everywhere:
            for p in range(positions):
                sent(k, p, side_sem)

    @pl.when(jnp.logical_not(end))
    def _():
        for p in range(PIECES):
            for kind in range(3):
                token_copy(guest, tp, p, kind, side).wait_send()
        for e in hosted:
            for h in range(HALVES):
                send_back(e, h).wait_send()
        for k in range(len(chunks)):
            sent(k, z + out, in_sem)
            for p in range(positions):
                sent(k, p, side_sem)
        for k in everywhere:
            sent(k, z, out_sem)
            sent(k, z - out, out_sem)
            sent(k, z - 2 * out, out_sem)


def streamed(groups, tps, tokens, gain, router, routes, w_gate, w_up, w_down):
    rows, depth = tokens.shape
    experts, shard, width = w_gate.shape
    down_rows, cols = w_down.shape[1:]
    positions = groups // CORES
    vmem = pl.BlockSpec(memory_space=pltpu.VMEM)
    hbm = pl.BlockSpec(memory_space=pl.ANY)
    chunks = (2 + HALVES) * experts
    dma = pltpu.SemaphoreType.DMA
    return pl.pallas_call(
        functools.partial(kernel, groups, tps, HOSTED),
        out_shape=jax.ShapeDtypeStruct((rows, cols), jnp.bfloat16),
        in_specs=[hbm, vmem, vmem, vmem, hbm, hbm, hbm],
        out_specs=vmem,
        scratch_shapes=[
            pltpu.VMEM((rows, depth), jnp.bfloat16),
            pltpu.VMEM((rows, depth), jnp.bfloat16),
            pltpu.VMEM((rows, depth), jnp.bfloat16),
            pltpu.VMEM((2, experts, groups, shard, width), jnp.bfloat16),
            pltpu.VMEM((experts, groups, down_rows, cols), jnp.bfloat16),
            pltpu.VMEM((experts, tps, rows, width), jnp.bfloat16),
            pltpu.VMEM((experts, rows, width), jnp.bfloat16),
            pltpu.VMEM((rows, router.shape[1]), jnp.float32),
            pltpu.VMEM((rows, cols), jnp.float32),
            dma,
            dma((chunks,)),
            dma((chunks, groups)),
            dma((chunks, positions)),
            dma((chunks, positions)),
            dma((chunks, positions)),
            dma((experts, HALVES, 3)),
            dma((experts, HALVES, tps)),
            dma((3, PIECES)),
            dma((tps, PIECES)),
            dma((experts, HALVES)),
            dma((experts, HALVES)),
        ],
        compiler_params=pltpu.CompilerParams(
            collective_id=0, has_side_effects=True, vmem_limit_bytes=60 * 1024 * 1024
        ),
    )(tokens, gain.reshape(1, -1), router.T, routes.T, w_gate, w_up, w_down)


def solution(mesh):
    groups, tps = mesh.shape["dp"], mesh.shape["tp"]
    fits = groups == 4 * CORES and tps == 4
    body = functools.partial(streamed, groups, tps) if fits else gathered
    return jax.shard_map(
        body,
        mesh=mesh,
        in_specs=(
            P("dp", None),
            P(),
            P(),
            P("dp", None),
            P(None, "dp", "tp"),
            P(None, "dp", "tp"),
            P(None, "dp", "tp"),
        ),
        out_specs=P("dp", "tp"),
        check_vma=False,
    )
```

```python
import functools

import jax
import jax.numpy as jnp
from jax import lax
from jax.experimental import pallas as pl
from jax.experimental.pallas import tpu as pltpu
from jax.sharding import PartitionSpec as P

EPS = 1e-06
ROUTE_SCALE = 2.5
MESH = pl.DeviceIdType.MESH
CORES = 2
PIECES = 4
HALVES = 2
HOSTED = (0, 1)


def gathered(tokens, gain, router, routes, w_gate, w_up, w_down):
    values = tokens.astype(jnp.float32)
    square = jnp.mean(values * values, axis=-1, keepdims=True)
    normed = (values * lax.rsqrt(square + EPS) * gain).astype(jnp.bfloat16)
    scores = jax.nn.sigmoid(
        jnp.dot(normed.astype(jnp.float32), router, precision=lax.Precision.HIGHEST)
    )
    labels = jnp.arange(router.shape[1], dtype=jnp.int32)
    picked_mask = (routes[:, :, None] == labels[None, None, :]).astype(jnp.float32)
    picked = jnp.sum(picked_mask * scores[:, None, :], axis=-1)
    chosen = jnp.sum(picked_mask, axis=1)
    combine = chosen * scores * ROUTE_SCALE / jnp.sum(picked, axis=-1, keepdims=True)
    held_weights = combine[:, : w_gate.shape[0]]
    full_gate, full_up, full_down = (
        lax.all_gather(w_gate, "dp", axis=1, tiled=True),
        lax.all_gather(w_up, "dp", axis=1, tiled=True),
        lax.all_gather(w_down, "dp", axis=1, tiled=True),
    )
    gate_value = jnp.einsum("td,edf->tef", normed, full_gate, preferred_element_type=jnp.float32)
    up_value = jnp.einsum("td,edf->tef", normed, full_up, preferred_element_type=jnp.float32)
    hidden = (jax.nn.silu(gate_value) * up_value * held_weights[:, :, None]).astype(jnp.bfloat16)
    whole_hidden = lax.all_gather(hidden, "tp", axis=2, tiled=True)
    mixed = jnp.einsum("tef,efd->td", whole_hidden, full_down, preferred_element_type=jnp.float32)
    return mixed.astype(jnp.bfloat16)


def kernel(
    groups, tps, hosted, x_hbm, gain_ref, router_ref, routes_ref, wg_hbm, wu_hbm, wd_hbm, o_ref,
    x, guest, guest_normed, w, dn, hid, guest_hid, comb, total,
    x_sem, own_sem, recv_sem, in_sem, out_sem, side_sem, hid_send, hid_recv,
    tok_send, tok_recv, back_send, back_recv,
):
    dp, tp = lax.axis_index("dp"), lax.axis_index("tp")
    positions = groups // CORES
    z, core = dp // CORES, dp % CORES
    experts = wg_hbm.shape[0]
    rows = x.shape[0]
    end = jnp.logical_or(z == positions - 1, z == 0)
    out = 2 * (2 * z // positions) - 1

    def at(p):
        return (p * CORES + core, tp)

    inner = at(z - out)
    outer = at(jnp.clip(z + out, 0, positions - 1))
    side = (z * CORES + (1 - core), tp)
    along_x = tp + 1 - 2 * (tp % 2)
    along_y = lax.rem(tp + 2, tps)
    across = lax.rem(along_x + 2, tps)

    load_x = pltpu.make_async_copy(x_hbm, x, x_sem)
    load_x.start()
    order = sorted(range(experts), key=lambda e: e not in hosted)
    chunks = [(m, e, 0) for e in order for m in (0, 1)]
    feeds = list(range(len(chunks)))
    chunks += [(2, e, h) for e in order for h in range(HALVES)]
    downs = [k for k in range(len(chunks)) if k not in feeds]
    everywhere = [k for k, (m, e, _) in enumerate(chunks) if m == 2 or e not in hosted]
    half = dn.shape[2] // HALVES
    strip = rows // HALVES

    def source(k):
        m, e, h = chunks[k]
        return wd_hbm.at[e, pl.ds(h * half, half)] if m == 2 else (wg_hbm, wu_hbm)[m].at[e]

    def slot(k, d):
        m, e, h = chunks[k]
        return dn.at[e, d, pl.ds(h * half, half)] if m == 2 else w.at[m, e, d]

    def copy_own(k):
        return pltpu.make_async_copy(source(k), slot(k, dp), own_sem.at[k])

    for k in range(len(chunks)):
        copy_own(k).start()

    barrier = pltpu.get_barrier_semaphore()
    pl.semaphore_signal(barrier, inc=1, device_id=side, device_id_type=MESH)
    pl.semaphore_signal(barrier, inc=1, device_id=inner, device_id_type=MESH)
    for i in range(1, tps):
        pl.semaphore_signal(
            barrier, inc=1, device_id=(dp, lax.rem(tp + i, tps)), device_id_type=MESH
        )

    @pl.when(jnp.logical_not(end))
    def _():
        pl.semaphore_signal(barrier, inc=1, device_id=outer, device_id_type=MESH)

    pl.semaphore_wait(barrier, tps + 2 - jnp.where(end, 1, 0))

    def send(k, d, src, sem, to):
        return pltpu.make_async_remote_copy(
            src_ref=src, dst_ref=slot(k, d), send_sem=sem.at[k, d // CORES],
            recv_sem=recv_sem.at[k, d], device_id=to, device_id_type=MESH,
        )

    def arrived(k, d):
        send(k, d, slot(k, d), side_sem, side).wait_recv()

    def pass_on(k, p, targets):
        d = p * CORES + core
        arrived(k, d)
        for sem, to in targets:
            send(k, d, slot(k, d), sem, to).start()

    def wait_side(k):
        for p in range(positions):
            arrived(k, p * CORES + (1 - core))
        copy_own(k).wait()

    quarter = rows // tps
    piece = quarter // PIECES

    def token_part(q, p):
        return pl.ds(pl.multiple_of(q * quarter + p * piece, piece), piece)

    def token_copy(src, q, p, kind, to):
        return pltpu.make_async_remote_copy(
            src_ref=src.at[token_part(q, p)], dst_ref=guest.at[token_part(q, p)],
            send_sem=tok_send.at[kind, p], recv_sem=tok_recv.at[q, p],
            device_id=to, device_id_type=MESH,
        )

    def token_arrived(q, p):
        token_copy(guest, q, p, 0, side).wait_recv()

    def norm(src, dst, start, count, steps):
        step = count // steps

        def body(i, _):
            part = pl.ds(pl.multiple_of(start + i * step, step), step)
            v = src[part, :].astype(jnp.float32)
            square = jnp.mean(v * v, axis=-1, keepdims=True)
            dst[part, :] = (v * lax.rsqrt(square + EPS) * gain_ref[...]).astype(jnp.bfloat16)
            return 0

        lax.fori_loop(0, steps, body, 0)

    def norm_quarter(q):
        norm(guest, guest_normed, q * quarter, quarter, 2)

    def score():
        rest = router_ref[...]
        logits = jnp.zeros((rows, rest.shape[0]), jnp.float32)
        parts = []
        for _ in range(3):
            part = rest.astype(jnp.bfloat16)
            rest = rest - part.astype(jnp.float32)
            parts.append(part)
        for part in parts[::-1]:
            logits += lax.dot_general(
                x[...], part, (((1,), (1,)), ((), ())), preferred_element_type=jnp.float32
            )
        scores = 1.0 / (1.0 + jnp.exp(-logits))
        routed = scores.shape[1]
        picks = routes_ref[...].astype(jnp.float32)
        labels = lax.broadcasted_iota(jnp.int32, scores.shape, 1).astype(jnp.float32)
        chosen = jnp.zeros_like(scores)
        for i in range(routes_ref.shape[0]):
            column = jnp.transpose(jnp.broadcast_to(picks[i : i + 1, :], (128, rows)))
            chosen += jnp.where(column[:, :routed] == labels, 1.0, 0.0)
        picked = chosen * scores
        comb[...] = picked * ROUTE_SCALE / jnp.sum(picked, axis=-1, keepdims=True)

    def hidden_copy(e, h, t, kind, to):
        part = pl.ds(h * strip, strip)
        return pltpu.make_async_remote_copy(
            src_ref=hid.at[e, t, part], dst_ref=hid.at[e, t, part],
            send_sem=hid_send.at[e, h, kind], recv_sem=hid_recv.at[e, h, t],
            device_id=(dp, to), device_id_type=MESH,
        )

    def share_hidden(e, h):
        hidden_copy(e, h, tp, 0, along_x).start()
        hidden_copy(e, h, tp, 1, along_y).start()

    def relay_hidden(e):
        for h, (t, to) in enumerate(((along_x, along_y), (along_y, along_x))):
            hidden_copy(e, h, t, 2, to).wait_recv()
            hidden_copy(e, h, t, 2, to).start()

    def wait_hidden(e):
        for h, t in ((0, along_y), (1, along_x), (0, across), (1, across)):
            hidden_copy(e, h, t, 2, along_x).wait_recv()

    def send_back(e, h):
        part = pl.ds(h * strip, strip)
        return pltpu.make_async_remote_copy(
            src_ref=guest_hid.at[e, part], dst_ref=hid.at[e, tp, part],
            send_sem=back_send.at[e, h], recv_sem=back_recv.at[e, h],
            device_id=outer, device_id_type=MESH,
        )

    def expert_hidden(e, h, src, dst):
        part = pl.ds(h * strip, strip)
        lhs = src[part, :]
        depth = x.shape[1]
        gate = jnp.dot(
            lhs, w[0, e].reshape(depth, w.shape[-1]), preferred_element_type=jnp.float32
        )
        up = jnp.dot(
            lhs, w[1, e].reshape(depth, w.shape[-1]), preferred_element_type=jnp.float32
        )
        dst[part, :] = (gate / (1.0 + jnp.exp(-gate)) * up).astype(jnp.bfloat16)

    def own_hidden(e):
        for h in range(HALVES):
            expert_hidden(e, h, x, hid.at[e, tp])
            share_hidden(e, h)

    def guest_hidden(e):
        for h in range(HALVES):
            expert_hidden(e, h, guest_normed, guest_hid.at[e])
            send_back(e, h).start()

    def sides_of(e):
        for k in feeds:
            if chunks[k][1] == e:
                wait_side(k)

    def down(e):
        cols = o_ref.shape[1]
        step = cols // 4
        wait_hidden(e)
        for k in downs:
            if chunks[k][1] == e:
                wait_side(k)

        def body(i, _):
            part = pl.ds(pl.multiple_of(i * step, step), step)
            lhs = jnp.concatenate([hid[e, t] for t in range(tps)], axis=1)
            rhs = dn[e, :, :, part].reshape(lhs.shape[1], step)
            term = jnp.dot(lhs, rhs, preferred_element_type=jnp.float32)
            term = term * comb[:, e : e + 1]
            if e != order[0]:
                term += total[:, part]
            if e == order[-1]:
                o_ref[:, part] = term.astype(o_ref.dtype)
            else:
                total[:, part] = term
            return 0

        lax.fori_loop(0, 4, body, 0)

    to_in, to_out, to_side = (in_sem, inner), (out_sem, outer), (side_sem, side)

    @pl.when(end)
    def _():
        for p in range(PIECES):
            token_copy(x_hbm, tp, p, 0, inner).start()
        for k in range(len(chunks)):
            send(k, dp, source(k), *to_in).start()
        for k in everywhere:
            send(k, dp, source(k), *to_side).start()
        load_x.wait()
        norm(x, x, 0, rows, 8)
        score()
        for k in everywhere:
            pass_on(k, z - out, [to_side])
        for k in everywhere[:-1]:
            pass_on(k, z - 2 * out, [to_side])
        for e in order:
            if e in hosted:
                for h in range(HALVES):
                    send_back(e, h).wait_recv()
                    share_hidden(e, h)
                relay_hidden(e)
        pass_on(everywhere[-1], z - 2 * out, [to_side])
        for e in order:
            if e not in hosted:
                for k in feeds:
                    if chunks[k][1] == e:
                        pass_on(k, z - 3 * out, [to_side])
                sides_of(e)
                own_hidden(e)
                relay_hidden(e)
        for e in order:
            for k in downs:
                if chunks[k][1] == e:
                    pass_on(k, z - 3 * out, [to_side])
            down(e)
        for k in range(len(chunks)):
            if k not in everywhere:
                copy_own(k).wait()

    @pl.when(jnp.logical_not(end))
    def _():
        def beyond(k):
            return [to_out] if k in everywhere else []

        for k in range(len(chunks) - 1):
            send(k, dp, source(k), *to_in).start()
        for k in everywhere:
            send(k, dp, source(k), *to_out).start()
        for k in range(len(chunks)):
            send(k, dp, source(k), *to_side).start()

        def from_outer(k):
            pass_on(k, z + out, [to_in, to_side])

        def from_near(k):
            pass_on(k, z - out, beyond(k) + [to_side])

        def from_far(k):
            pass_on(k, z - 2 * out, beyond(k) + [to_side])

        load_x.wait()
        norm(x, x, 0, rows, 8)
        score()
        for p in range(PIECES):
            token_arrived(tp, p)
            token_copy(guest, tp, p, 0, (dp, along_x)).start()
            token_copy(guest, tp, p, 1, (dp, along_y)).start()
            from_near(p)
        norm_quarter(tp)
        for p in range(PIECES):
            token_arrived(along_x, p)
            if p < PIECES // 2:
                token_copy(guest, along_x, p, 2, (dp, along_y)).start()
            token_arrived(along_y, p)
            if p >= PIECES // 2:
                token_copy(guest, along_y, p, 2, (dp, along_x)).start()
            if p == 0:
                from_near(downs[0])
                from_near(downs[1])
            if p == 1:
                from_near(downs[2])
            if p == 2:
                from_outer(feeds[0])
        norm_quarter(along_x)
        from_outer(feeds[1])
        norm_quarter(along_y)
        from_far(feeds[0])
        from_outer(feeds[2])
        for p in range(PIECES):
            token_arrived(across, p)
        norm_quarter(across)
        from_far(feeds[1])
        sides_of(order[0])
        own_hidden(order[0])
        from_outer(feeds[3])
        send(len(chunks) - 1, dp, source(len(chunks) - 1), *to_in).start()
        guest_hidden(order[0])
        from_far(feeds[2])
        from_outer(downs[0])
        from_outer(downs[1])
        relay_hidden(order[0])
        from_far(feeds[3])
        sides_of(order[1])
        if order[1] in hosted:
            guest_hidden(order[1])
        from_outer(downs[2])
        from_near(downs[3])
        own_hidden(order[1])
        from_outer(downs[3])
        for k in downs:
            from_far(k)
        relay_hidden(order[1])
        for e in order:
            down(e)

    def sent(k, p, sem):
        d = p * CORES + core
        send(k, d, slot(k, d), sem, side).wait_send()

    for e in range(experts):
        for h in range(HALVES):
            for kind in range(3):
                hidden_copy(e, h, tp, kind, along_x).wait_send()
    for k in range(len(chunks)):
        sent(k, z, in_sem)

    @pl.when(end)
    def _():
        for p in range(PIECES):
            token_copy(x_hbm, tp, p, 0, inner).wait_send()
        for k in everywhere:
            for p in range(positions):
                sent(k, p, side_sem)

    @pl.when(jnp.logical_not(end))
    def _():
        for p in range(PIECES):
            for kind in range(3):
                token_copy(guest, tp, p, kind, side).wait_send()
        for e in hosted:
            for h in range(HALVES):
                send_back(e, h).wait_send()
        for k in range(len(chunks)):
            sent(k, z + out, in_sem)
            for p in range(positions):
                sent(k, p, side_sem)
        for k in everywhere:
            sent(k, z, out_sem)
            sent(k, z - out, out_sem)
            sent(k, z - 2 * out, out_sem)


def streamed(groups, tps, tokens, gain, router, routes, w_gate, w_up, w_down):
    rows, depth = tokens.shape
    experts, shard, width = w_gate.shape
    down_rows, cols = w_down.shape[1:]
    positions = groups // CORES
    vmem = pl.BlockSpec(memory_space=pltpu.VMEM)
    hbm = pl.BlockSpec(memory_space=pl.ANY)
    chunks = (2 + HALVES) * experts
    dma = pltpu.SemaphoreType.DMA
    return pl.pallas_call(
        functools.partial(kernel, groups, tps, HOSTED),
        out_shape=jax.ShapeDtypeStruct((rows, cols), jnp.bfloat16),
        in_specs=[hbm, vmem, vmem, vmem, hbm, hbm, hbm],
        out_specs=vmem,
        scratch_shapes=[
            pltpu.VMEM((rows, depth), jnp.bfloat16),
            pltpu.VMEM((rows, depth), jnp.bfloat16),
            pltpu.VMEM((rows, depth), jnp.bfloat16),
            pltpu.VMEM((2, experts, groups, shard, width), jnp.bfloat16),
            pltpu.VMEM((experts, groups, down_rows, cols), jnp.bfloat16),
            pltpu.VMEM((experts, tps, rows, width), jnp.bfloat16),
            pltpu.VMEM((experts, rows, width), jnp.bfloat16),
            pltpu.VMEM((rows, router.shape[1]), jnp.float32),
            pltpu.VMEM((rows, cols), jnp.float32),
            dma,
            dma((chunks,)),
            dma((chunks, groups)),
            dma((chunks, positions)),
            dma((chunks, positions)),
            dma((chunks, positions)),
            dma((experts, HALVES, 3)),
            dma((experts, HALVES, tps)),
            dma((3, PIECES)),
            dma((tps, PIECES)),
            dma((experts, HALVES)),
            dma((experts, HALVES)),
        ],
        compiler_params=pltpu.CompilerParams(
            collective_id=0, has_side_effects=True, vmem_limit_bytes=60 * 1024 * 1024
        ),
    )(tokens, gain.reshape(1, -1), router.T, routes.T, w_gate, w_up, w_down)


def solution(mesh):
    groups, tps = mesh.shape["dp"], mesh.shape["tp"]
    fits = groups == 4 * CORES and tps == 4
    body = functools.partial(streamed, groups, tps) if fits else gathered
    return jax.shard_map(
        body,
        mesh=mesh,
        in_specs=(
            P("dp", None),
            P(),
            P(),
            P("dp", None),
            P(None, "dp", "tp"),
            P(None, "dp", "tp"),
            P(None, "dp", "tp"),
        ),
        out_specs=P("dp", "tp"),
        check_vma=False,
    )
```
